256 devices in a mesh: chan: 2 (over y_hi), seq: 16 (over z, core), dp: 8 (over x, y_lo).
Axes of the slice: x: 4, y: 4 (y_hi: 2, y_lo: 2; y = y_hi * 2 + y_lo), z: 8, core: 2. Of those that a mesh axis runs over, the one named last changes fastest.
Arguments:
- queries: bfloat16 [8, 2, 2048, 2048], P('dp', 'chan', 'seq'), may hold values from -8 to 8
- keys: bfloat16 [8, 2, 2048, 2048], P('dp', 'chan', 'seq'), may hold values from -8 to 8
- values: bfloat16 [8, 2, 2048, 2048], P('dp', 'chan', 'seq'), may hold values from -6 to 6
- out_grad: bfloat16 [8, 2, 2048, 2048], P('dp', 'chan', 'seq'), may hold values from -6 to 6
- cross_bias: float32 [16], replicated, may hold values from -2 to 2
- lengths: int32 [8], P('dp'), may hold values from 512 to 2048
Outputs:
- query_grad: bfloat16 [8, 2, 2048, 2048], P('dp', 'chan', 'seq')
- key_grad: bfloat16 [8, 2, 2048, 2048], P('dp', 'chan', 'seq')
- value_grad: bfloat16 [8, 2, 2048, 2048], P('dp', 'chan', 'seq')
- bias_grad: float32 [16], replicated
The draws below stay inside these ranges and needn't reach their ends.
Inputs may be any that keep to these rules, and one draw needn't show every extreme that they name: Frames of conversation b from lengths[b] on are padding in both channels.
All inputs are finite; a program needn't handle non-finite values.
Results may differ from the reference program's by a relative error of at most 0.011.
Values may be sent and summed in bfloat16 or wider, within the bound.
A program may use at most 128 MiB of HBM per device.

```python
import math
import jax
import jax.numpy as jnp
from jax import lax

TOK_DEV = 128
HEADS = 16
HEAD_DIM = 128
LOOKBACK = 6
FRAMES = 2048
CONVS = 8
N_SEQ = 16


def aligned_pattern(key):
    array_shape = (CONVS, 2, FRAMES, HEADS * HEAD_DIM)
    sign_table = jnp.where(jax.random.bernoulli(jax.random.fold_in(key, 11), 0.5, array_shape), 1.0, -1.0)
    position = jnp.arange(FRAMES, dtype=jnp.int32)
    marked = position % (2 * TOK_DEV) == TOK_DEV // 2
    level = (position // (2 * TOK_DEV) % 3).astype(jnp.float32)
    strength = 5.0 + 1.5 * level
    return (sign_table, marked, strength)


def background_draw(key, salt):
    array_shape = (CONVS, 2, FRAMES, HEADS * HEAD_DIM)
    return jnp.clip(jax.random.normal(jax.random.fold_in(key, salt), array_shape, jnp.float32), -5.0, 5.0)


def draw_queries(key, part):
    background = background_draw(key, 21)
    sign_table, marked, strength = aligned_pattern(key)
    planted = sign_table * strength[None, None, :, None]
    return jnp.where(marked[None, None, :, None], planted, background).astype(jnp.bfloat16)


def draw_keys(key, part):
    background = background_draw(key, 31)
    sign_table, marked, strength = aligned_pattern(key)
    planted = sign_table * strength[None, None, :, None]
    next_marked = jnp.roll(marked, -1)
    next_strength = jnp.roll(strength, -1)
    shrink = 1.0 - 2.0 / (next_strength * next_strength * HEAD_DIM ** 0.5)
    neighbour = jnp.roll(sign_table, -1, axis=2) * (next_strength * shrink)[None, None, :, None]
    result = jnp.where(next_marked[None, None, :, None], neighbour, background)
    result = jnp.where(marked[None, None, :, None], planted, result)
    return result.astype(jnp.bfloat16)


def plant(values, stream_key, least, high):
    dims = values.shape
    index_at = [jax.random.randint(jax.random.fold_in(stream_key, axis), (), 0, dims[axis]) for axis in range(len(dims))]
    values = values.at[tuple(index_at)].set(least)
    longest = dims.index(max(dims))
    index_at[longest] = (index_at[longest] + 1) % dims[longest]
    return values.at[tuple(index_at)].set(high)


def block_levels(own_key, shape, pieces, low, largest):
    def one(axis_at, shards_of):
        draws = jax.random.uniform(jax.random.fold_in(jax.random.fold_in(own_key, 6), axis_at), (shards_of,), jnp.float32, low / len(pieces), largest / len(pieces))
        return jnp.repeat(jnp.exp(draws), shape[axis_at] // shards_of).reshape((-1,) + (1,) * (len(shape) - axis_at - 1))

    gain = one(*pieces[0])
    for cut in pieces[1:]:
        gain = gain * one(*cut)
    return gain


def gaussian(stream_key, dims, width, bound, pieces=(), kind=jnp.bfloat16):
    gain = block_levels(stream_key, dims, pieces, -0.22, 0.18) if pieces else 1.0
    array = jax.random.normal(stream_key, dims, jnp.float32) * width * gain
    return jnp.minimum(jnp.maximum(array, -bound), bound).astype(kind)


def setup_inputs(seed: int = 0) -> dict:
    streams_of = jax.random.split(jax.random.key(seed), 7)
    return {
        "queries": draw_queries(jax.random.fold_in(streams_of[6], 71), 0),
        "keys": draw_keys(jax.random.fold_in(streams_of[6], 71), 0),
        "values": gaussian(streams_of[2], (CONVS, 2, FRAMES, HEADS * HEAD_DIM), 1.0, 6.0, ((0, 8), (1, 2), (2, 16))),
        "out_grad": gaussian(streams_of[3], (CONVS, 2, FRAMES, HEADS * HEAD_DIM), 1.0, 6.0, ((0, 8), (1, 2), (2, 16))),
        "cross_bias": jnp.clip(jax.random.uniform(streams_of[4], (HEADS,), jnp.float32, -2.0, 2.0), -2.0, 2.0),
        "lengths": plant(jax.random.randint(streams_of[5], (CONVS,), FRAMES // 4, FRAMES + 1), jax.random.fold_in(streams_of[5], 1), FRAMES // 4, FRAMES).astype(jnp.int32),
    }


NEG_FILL = -1e+30

def reference(queries, keys, values, out_grad, cross_bias, lengths):
    feature_width = HEADS * HEAD_DIM
    front_rows = LOOKBACK * TOK_DEV
    window_rows = (LOOKBACK + 1) * TOK_DEV
    root_scale = 1.0 / math.sqrt(HEAD_DIM)
    highest = lax.Precision.HIGHEST

    def conversation(packed):
        query_all, key_all, value_all, grad_all, dialog_length = packed
        key_pad = jnp.pad(key_all, ((0, 0), (front_rows, 0), (0, 0)))
        value_pad = jnp.pad(value_all, ((0, 0), (front_rows, 0), (0, 0)))

        def block_step(carried, block_index):
            key_sum, value_sum, bias_sum = carried
            first_frame = (block_index * TOK_DEV).astype(jnp.int32)
            query_block = lax.dynamic_slice_in_dim(query_all, first_frame, TOK_DEV, 1)
            grad_block = lax.dynamic_slice_in_dim(grad_all, first_frame, TOK_DEV, 1)
            key_block = lax.dynamic_slice_in_dim(key_pad, first_frame, window_rows, 1)
            value_block = lax.dynamic_slice_in_dim(value_pad, first_frame, window_rows, 1)
            query_heads = query_block.reshape(2 * TOK_DEV, HEADS, HEAD_DIM).astype(jnp.float32)
            grad_heads = grad_block.reshape(2 * TOK_DEV, HEADS, HEAD_DIM).astype(jnp.float32)
            key_heads = key_block.reshape(2 * window_rows, HEADS, HEAD_DIM).astype(jnp.float32)
            value_heads = value_block.reshape(2 * window_rows, HEADS, HEAD_DIM).astype(jnp.float32)
            query_frame = jnp.tile(first_frame + jnp.arange(TOK_DEV, dtype=jnp.int32), 2)
            key_frame = jnp.tile(first_frame - front_rows + jnp.arange(window_rows, dtype=jnp.int32), 2)
            tower_index = jnp.arange(2 * TOK_DEV, dtype=jnp.int32) // TOK_DEV
            key_channel = jnp.arange(2 * window_rows, dtype=jnp.int32) // window_rows
            partner = (tower_index[:, None] != key_channel[None, :]).astype(jnp.float32)
            allowed = (key_frame[None, :] > query_frame[:, None] - front_rows) & (key_frame[None, :] <= query_frame[:, None])
            allowed = allowed & (key_frame[None, :] >= 0) & (key_frame[None, :] < dialog_length)
            allowed = allowed & (query_frame[:, None] < dialog_length)
            scores = jnp.einsum('phd,shd->hps', query_heads, key_heads, precision=highest) * root_scale
            scores = scores + cross_bias[:, None, None] * partner[None]
            scores = jnp.where(allowed[None], scores, NEG_FILL)
            row_max = lax.optimization_barrier(jnp.max(scores, axis=2))
            row_total = lax.optimization_barrier(jnp.sum(jnp.where(allowed[None], jnp.exp(scores - row_max[:, :, None]), 0.0), axis=2))
            log_norm = row_max + jnp.log(jnp.where(row_total > 0.0, row_total, 1.0))
            weights = jnp.where(allowed[None], jnp.exp(scores - log_norm[:, :, None]), 0.0)
            weight_grad = jnp.einsum('phd,shd->hps', grad_heads, value_heads, precision=highest)
            row_delta = lax.optimization_barrier(jnp.sum(weights * weight_grad, axis=2))
            score_grad = weights * (weight_grad - row_delta[:, :, None])
            weight_low = lax.optimization_barrier(weights.astype(jnp.bfloat16)).astype(jnp.float32)
            score_low = lax.optimization_barrier(score_grad.astype(jnp.bfloat16)).astype(jnp.float32)
            query_term = jnp.einsum('hps,shd->phd', score_low, key_heads, precision=highest) * root_scale
            key_term = jnp.einsum('hps,phd->shd', score_low, query_heads, precision=highest) * root_scale
            value_term = jnp.einsum('hps,phd->shd', weight_low, grad_heads, precision=highest)
            bias_term = lax.optimization_barrier(jnp.sum(score_grad * partner[None], axis=(1, 2)))
            key_old = lax.dynamic_slice_in_dim(key_sum, first_frame, window_rows, 1)
            value_old = lax.dynamic_slice_in_dim(value_sum, first_frame, window_rows, 1)
            key_sum = lax.dynamic_update_slice_in_dim(key_sum, key_old + key_term.reshape(2, window_rows, feature_width), first_frame, 1)
            value_sum = lax.dynamic_update_slice_in_dim(value_sum, value_old + value_term.reshape(2, window_rows, feature_width), first_frame, 1)
            query_out = query_term.reshape(2, TOK_DEV, feature_width).astype(jnp.bfloat16)
            return ((key_sum, value_sum, bias_sum + bias_term), query_out)
        initial = (jnp.zeros((2, front_rows + FRAMES, feature_width), jnp.float32), jnp.zeros((2, front_rows + FRAMES, feature_width), jnp.float32), jnp.zeros((HEADS,), jnp.float32))
        finals, query_blocks = lax.scan(block_step, initial, jnp.arange(N_SEQ, dtype=jnp.int32))
        key_sum, value_sum, bias_sum = finals
        query_whole = jnp.transpose(query_blocks, (1, 0, 2, 3)).reshape(2, FRAMES, feature_width)
        return (query_whole, key_sum[:, front_rows:].astype(jnp.bfloat16), value_sum[:, front_rows:].astype(jnp.bfloat16), bias_sum)
    results = lax.map(conversation, (queries, keys, values, out_grad, lengths))
    return (results[0], results[1], results[2], lax.optimization_barrier(jnp.sum(results[3], axis=0)))
```

```python
import functools
import math

import jax
import jax.numpy as jnp
from jax import lax
from jax.experimental import pallas as pl
from jax.experimental.pallas import tpu as pltpu
from jax.sharding import PartitionSpec as P

BLOCK = 128
WINDOW = 7
CHIPS = 8
NEG_FILL = -1e30
MESH = pl.DeviceIdType.MESH
NT = (((1,), (1,)), ((), ()))
NN = (((1,), (0,)), ((), ()))
TN = (((0,), (0,)), ((), ()))
BF = jnp.bfloat16
F32 = jnp.float32


def dot(a, b, dims):
    return lax.dot_general(a, b, dims, preferred_element_type=F32)


def kernel(
    heads,
    lengths,
    bias,
    q_hbm,
    k_hbm,
    v_hbm,
    g_hbm,
    dq_hbm,
    dk_hbm,
    dv_hbm,
    bias_out,
    kv,
    qg,
    tri,
    prob,
    wgrad,
    terms,
    side_out,
    side_in,
    chain_out,
    chain_in,
    dq_own,
    dq_send,
    dq_recv,
    dq_stage,
    out_stage,
    stat_out,
    stat_in,
    load_sem,
    hop_s,
    hop_r,
    side_s,
    side_r,
    swap_s,
    swap_r,
    stat_s,
    stat_r,
    term_s,
    term_r,
    chain_s,
    chain_r,
    dq_s,
    dq_r,
    store_sem,
):
    root_scale = 1.0 / math.sqrt(BLOCK)
    chan = lax.axis_index("chan")
    seq = lax.axis_index("seq")
    chip = lax.div(seq, 2)
    core = lax.rem(seq, 2)
    mate = {"seq": seq + 1 - 2 * core}
    partner = {"chan": 1 - chan}
    above = {"seq": lax.rem(seq + 2, 2 * CHIPS)}
    below = {"seq": lax.rem(seq + 2 * CHIPS - 2, 2 * CHIPS)}
    has_above = chip < CHIPS - 1

    def remote(src, dst, send, recv, where):
        return pltpu.make_async_remote_copy(
            src_ref=src, dst_ref=dst, send_sem=send, recv_sem=recv, device_id=where, device_id_type=MESH
        )

    def loads(j):
        cols = pl.ds(pl.multiple_of(j * BLOCK, BLOCK), BLOCK)
        own = pl.ds(0, BLOCK)
        return (
            pltpu.make_async_copy(k_hbm.at[0, 0, :, cols], kv.at[0, j, 0], load_sem.at[0, j]),
            pltpu.make_async_copy(v_hbm.at[0, 0, :, cols], kv.at[0, j, 1], load_sem.at[1, j]),
            pltpu.make_async_copy(q_hbm.at[0, 0, :, cols], qg.at[j, 0, own], load_sem.at[2, j]),
            pltpu.make_async_copy(g_hbm.at[0, 0, :, cols], qg.at[j, 1, own], load_sem.at[3, j]),
        )

    def stores(j):
        cols = pl.ds(pl.multiple_of(j * BLOCK, BLOCK), BLOCK)
        return (
            pltpu.make_async_copy(out_stage.at[j, 0], dk_hbm.at[0, 0, :, cols], store_sem.at[0, j]),
            pltpu.make_async_copy(out_stage.at[j, 1], dv_hbm.at[0, 0, :, cols], store_sem.at[1, j]),
        )

    def store_query(j):
        cols = pl.ds(pl.multiple_of(j * BLOCK, BLOCK), BLOCK)
        return pltpu.make_async_copy(dq_stage.at[j], dq_hbm.at[0, 0, :, cols], store_sem.at[2, j])

    def hop(n, j):
        return remote(kv.at[2 * n - 2, j], kv.at[2 * n, j], hop_s.at[n - 1, j], hop_r.at[n - 1, j], above)

    def side(n, j):
        i = n - core
        return remote(kv.at[2 * n, j], kv.at[2 * i + 1, j], side_s.at[i, j], side_r.at[i, j], mate)

    def side_arrival(i, j):
        return remote(kv.at[2 * i + 1, j], kv.at[2 * i + 1, j], side_s.at[i, j], side_r.at[i, j], mate)

    def swap(j):
        return remote(
            qg.at[j, :, pl.ds(0, BLOCK)], qg.at[j, :, pl.ds(BLOCK, BLOCK)], swap_s.at[j], swap_r.at[j], partner
        )

    def stat(j):
        return remote(stat_out.at[j], stat_in.at[j], stat_s.at[j], stat_r.at[j], partner)

    def term(i, j):
        h = i + 1 - core
        return remote(side_out.at[i, j], side_in.at[h, j], term_s.at[i, j], term_r.at[h, j], mate)

    def term_arrival(h, j):
        return remote(side_in.at[h, j], side_in.at[h, j], term_s.at[0, j], term_r.at[h, j], mate)

    def chain(h, j):
        return remote(
            chain_out.at[h - 1, j], chain_in.at[h - 1, j], chain_s.at[h - 1, j], chain_r.at[h - 1, j], below
        )

    def query(j):
        return remote(dq_send.at[j], dq_recv.at[j], dq_s.at[j], dq_r.at[j], partner)

    def fetch(j, _):
        for copy in loads(j):
            copy.start()
        return 0

    lax.fori_loop(0, heads, fetch, 0)

    barrier = pltpu.get_barrier_semaphore()
    pl.semaphore_signal(barrier, inc=1, device_id=mate, device_id_type=MESH)
    pl.semaphore_signal(barrier, inc=1, device_id=partner, device_id_type=MESH)

    @pl.when(has_above)
    def _():
        pl.semaphore_signal(barrier, inc=1, device_id=above, device_id_type=MESH)

    @pl.when(chip > 0)
    def _():
        pl.semaphore_signal(barrier, inc=1, device_id=below, device_id_type=MESH)

    key_row = lax.broadcasted_iota(jnp.int32, (BLOCK, 2 * BLOCK), 0)
    query_col = lax.rem(lax.broadcasted_iota(jnp.int32, (BLOCK, 2 * BLOCK), 1), BLOCK)
    absent = [jnp.where(seq >= d, 0.0, NEG_FILL).astype(F32) for d in range(WINDOW)]
    tri[0] = jnp.where(key_row <= query_col, 0.0, NEG_FILL)
    tri[1] = jnp.where(key_row > query_col, 0.0, NEG_FILL) + absent[WINDOW - 1]
    lane = lax.rem(lax.broadcasted_iota(jnp.int32, (1, 2 * BLOCK), 1), BLOCK)
    valid = jnp.where(seq * BLOCK + lane < lengths[0], 1.0, 0.0).astype(F32)
    crossed = lax.broadcasted_iota(jnp.int32, (1, 2 * BLOCK), 1) >= BLOCK

    def clear(j, _):
        nothing = jnp.zeros((2, BLOCK, BLOCK), BF)
        for d in range(1, WINDOW):

            @pl.when(seq < d)
            def _():
                kv[d, j] = nothing

        @pl.when(core == 0)
        def _():
            side_in[3, j] = nothing

        @pl.when(core == 1)
        def _():
            side_in[0, j] = nothing

        @pl.when(jnp.logical_not(has_above))
        def _():
            for h in range(3):
                chain_in[h, j] = nothing

        return 0

    lax.fori_loop(0, heads, clear, 0)

    pl.semaphore_wait(barrier, 2 + jnp.where(has_above, 1, 0) + jnp.where(chip > 0, 1, 0))

    def forward(j):
        swap(j).wait_recv()
        for i in range(3):

            @pl.when(seq >= 2 * i + 1)
            def _():
                side_arrival(i, j).wait_recv()

        queries, grads = qg[j, 0], qg[j, 1]
        peak = None
        for d in range(WINDOW):
            score = dot(kv[d, j, 0], queries, NT) * root_scale
            if d == 0:
                score = score + tri[0]
            elif d == WINDOW - 1:
                score = score + tri[1]
            else:
                score = score + absent[d]
            prob[d] = score
            top = jnp.max(score, axis=0, keepdims=True)
            peak = top if peak is None else jnp.maximum(peak, top)
        total = moment = None
        for d in range(WINDOW):
            weight_grad = dot(kv[d, j, 1], grads, NT)
            weight = jnp.exp(prob[d] - peak)
            prob[d] = weight
            wgrad[d] = weight_grad
            a = jnp.sum(weight, axis=0, keepdims=True)
            b = jnp.sum(weight * weight_grad, axis=0, keepdims=True)
            total = a if total is None else total + a
            moment = b if moment is None else moment + b
        offset = jnp.where(crossed, bias[j], 0.0)
        stat_out[j, 0:1] = peak + offset
        stat_out[j, 1:2] = total
        stat_out[j, 2:3] = moment
        stat_out[j, 3:8] = jnp.zeros((5, 2 * BLOCK), F32)
        stat(j).start()

    def backward(j):
        stat(j).wait_recv()

        def turned(row):
            theirs = stat_in[j, row : row + 1]
            return jnp.concatenate([theirs[:, BLOCK:], theirs[:, :BLOCK]], axis=1)

        peak = stat_out[j, 0:1]
        their_peak = turned(0)
        merged = jnp.maximum(peak, their_peak)
        mine, theirs = jnp.exp(peak - merged), jnp.exp(their_peak - merged)
        own_total = stat_out[j, 1:2] * mine
        own_moment = stat_out[j, 2:3] * mine
        inverse = valid / (own_total + turned(1) * theirs)
        delta = (own_moment + turned(2) * theirs) * inverse
        rescale = mine * inverse
        bias_row = (own_moment - delta * own_total) * inverse
        bias_out[pl.ds(j, 1), :] = bias_row[:, BLOCK:]
        queries, grads = qg[j, 0], qg[j, 1]
        query_term = None
        for d in range(WINDOW):
            weight = prob[d] * rescale
            score_grad = (weight * (wgrad[d] - delta)).astype(BF)
            weight = weight.astype(BF)
            value_term = dot(weight, grads, NN)
            key_term = dot(score_grad, queries, NN) * root_scale
            part = dot(score_grad, kv[d, j, 0], TN)
            query_term = part if query_term is None else query_term + part
            if d % 2 == 0:
                terms[d // 2, j, 0] = key_term
                terms[d // 2, j, 1] = value_term
            else:
                side_out[d // 2, j, 0] = key_term.astype(BF)
                side_out[d // 2, j, 1] = value_term.astype(BF)
        query_term = query_term * root_scale
        dq_own[j] = query_term[:BLOCK]
        dq_send[j] = query_term[BLOCK:].astype(BF)
        for i in range(3):

            @pl.when(seq >= 2 * i + 1)
            def _():
                term(i, j).start()

        query(j).start()

    def within(j, action):
        @pl.when(jnp.logical_and(j >= 0, j < heads))
        def _():
            action(j)

    def send_own(j):
        for copy in loads(j):
            copy.wait()

        @pl.when(has_above)
        def _():
            hop(1, j).start()

        @pl.when(core == 0)
        def _():
            side(0, j).start()

        swap(j).start()

    def relay(n, j):
        @pl.when(chip >= n)
        def _():
            hop(n, j).wait_recv()
            if n < 3:

                @pl.when(has_above)
                def _():
                    hop(n + 1, j).start()

                side(n, j).start()
            else:

                @pl.when(core == 1)
                def _():
                    side(n, j).start()

    def finish_query(j):
        query(j).wait_recv()
        dq_stage[j] = (dq_own[j] + dq_recv[j].astype(F32)).astype(BF)
        store_query(j).start()

    def reduce(h, j):
        @pl.when(chip >= h)
        def _():
            if h == 3:
                pl.when(core == 1)(lambda: term_arrival(h, j).wait_recv())
            elif h == 0:
                pl.when(core == 0)(lambda: term_arrival(h, j).wait_recv())
            else:
                term_arrival(h, j).wait_recv()
            total = terms[h, j] + side_in[h, j].astype(F32)
            if h < 3:
                pl.when(has_above)(lambda: chain(h + 1, j).wait_recv())
                total = total + chain_in[h, j].astype(F32)
            if h > 0:
                chain_out[h - 1, j] = total.astype(BF)
                chain(h, j).start()
            else:
                out_stage[j] = total.astype(BF)
                for copy in stores(j):
                    copy.start()

    def step(i, _):
        within(i + 3, send_own)
        within(i + 2, functools.partial(relay, 1))
        within(i + 1, functools.partial(relay, 2))
        within(i, functools.partial(relay, 3))
        within(i - 1, backward)
        within(i, forward)
        within(i - 2, functools.partial(reduce, 3))
        within(i - 3, functools.partial(reduce, 2))
        within(i - 4, functools.partial(reduce, 1))
        within(i - 5, functools.partial(reduce, 0))
        within(i - 2, finish_query)
        return 0

    lax.fori_loop(-3, heads + 5, step, 0)

    def drain(j, _):
        swap(j).wait_send()
        stat(j).wait_send()
        query(j).wait_send()
        store_query(j).wait()
        for copy in stores(j):
            copy.wait()
        for n in range(1, 4):
            pl.when(jnp.logical_and(has_above, chip >= n - 1))(lambda: hop(n, j).wait_send())
        pl.when(core == 0)(lambda: side(0, j).wait_send())
        for n in (1, 2):
            pl.when(chip >= n)(lambda: side(n, j).wait_send())
        pl.when(jnp.logical_and(chip >= 3, core == 1))(lambda: side(3, j).wait_send())
        for i in range(3):
            pl.when(seq >= 2 * i + 1)(lambda: term(i, j).wait_send())
        for h in range(1, 4):
            pl.when(chip >= h)(lambda: chain(h, j).wait_send())
        return 0

    lax.fori_loop(0, heads, drain, 0)


def shards(queries, keys, values, out_grad, cross_bias, lengths):
    heads = cross_bias.shape[0]
    like = jax.ShapeDtypeStruct(queries.shape, BF)
    dma = pltpu.SemaphoreType.DMA
    anywhere = pl.BlockSpec(memory_space=pl.ANY)
    scalar = pl.BlockSpec(memory_space=pltpu.SMEM)
    tile = (BLOCK, BLOCK)
    wide = (BLOCK, 2 * BLOCK)
    query_grad, key_grad, value_grad, bias_rows = pl.pallas_call(
        functools.partial(kernel, heads),
        out_shape=(like, like, like, jax.ShapeDtypeStruct((heads, BLOCK), F32)),
        in_specs=[scalar, scalar] + [anywhere] * 4,
        out_specs=(anywhere, anywhere, anywhere, pl.BlockSpec(memory_space=pltpu.VMEM)),
        scratch_shapes=[
            pltpu.VMEM((WINDOW, heads, 2, *tile), BF),
            pltpu.VMEM((heads, 2, 2 * BLOCK, BLOCK), BF),
            pltpu.VMEM((2, *wide), F32),
            pltpu.VMEM((WINDOW, *wide), F32),
            pltpu.VMEM((WINDOW, *wide), F32),
            pltpu.VMEM((4, heads, 2, *tile), F32),
            pltpu.VMEM((3, heads, 2, *tile), BF),
            pltpu.VMEM((4, heads, 2, *tile), BF),
            pltpu.VMEM((3, heads, 2, *tile), BF),
            pltpu.VMEM((3, heads, 2, *tile), BF),
            pltpu.VMEM((heads, *tile), F32),
            pltpu.VMEM((heads, *tile), BF),
            pltpu.VMEM((heads, *tile), BF),
            pltpu.VMEM((heads, *tile), BF),
            pltpu.VMEM((heads, 2, *tile), BF),
            pltpu.VMEM((heads, 8, 2 * BLOCK), F32),
            pltpu.VMEM((heads, 8, 2 * BLOCK), F32),
            dma((4, heads)),
            dma((3, heads)),
            dma((3, heads)),
            dma((3, heads)),
            dma((3, heads)),
            dma((heads,)),
            dma((heads,)),
            dma((heads,)),
            dma((heads,)),
            dma((3, heads)),
            dma((4, heads)),
            dma((3, heads)),
            dma((3, heads)),
            dma((heads,)),
            dma((heads,)),
            dma((3, heads)),
        ],
        compiler_params=pltpu.CompilerParams(
            collective_id=0, has_side_effects=True, vmem_limit_bytes=56 * 1024 * 1024
        ),
    )(lengths, cross_bias, queries, keys, values, out_grad)
    bias_grad = lax.psum(jnp.sum(bias_rows, axis=1), ("chan", "seq", "dp"))
    return query_grad, key_grad, value_grad, bias_grad


def solution(mesh):
    split = P("dp", "chan", "seq", None)
    return jax.shard_map(
        shards,
        mesh=mesh,
        in_specs=(split, split, split, split, P(), P("dp")),
        out_specs=(split, split, split, P()),
        check_vma=False,
    )
```

```python
import functools
import math

import jax
import jax.numpy as jnp
from jax import lax
from jax.experimental import pallas as pl
from jax.experimental.pallas import tpu as pltpu
from jax.sharding import PartitionSpec as P

BLOCK = 128
WINDOW = 7
NEG_FILL = -1e30
MESH = pl.DeviceIdType.MESH
NT = (((1,), (1,)), ((), ()))
NN = (((1,), (0,)), ((), ()))
TN = (((0,), (0,)), ((), ()))
BF = jnp.bfloat16
F32 = jnp.float32


def dot(a, b, dims):
    return lax.dot_general(a, b, dims, preferred_element_type=F32)


def kernel(
    heads,
    chips,
    convs,
    lengths,
    bias,
    q_hbm,
    k_hbm,
    v_hbm,
    g_hbm,
    dq_hbm,
    dk_hbm,
    dv_hbm,
    bias_out,
    kv,
    qg,
    tri,
    prob,
    wgrad,
    terms,
    side_out,
    side_in,
    chain_out,
    chain_in,
    dq_own,
    dq_send,
    dq_recv,
    dq_stage,
    out_stage,
    stat_out,
    stat_in,
    bias_mate,
    bias_seq,
    bias_row,
    bias_col,
    load_sem,
    hop_s,
    hop_r,
    side_s,
    side_r,
    swap_s,
    swap_r,
    stat_s,
    stat_r,
    term_s,
    term_r,
    chain_s,
    chain_r,
    dq_s,
    dq_r,
    store_sem,
    mate_sem,
    seq_s,
    seq_r,
    row_s,
    row_r,
    col_s,
    col_r,
):
    root_scale = 1.0 / math.sqrt(BLOCK)
    chan = lax.axis_index("chan")
    seq = lax.axis_index("seq")
    chip = lax.div(seq, 2)
    core = lax.rem(seq, 2)
    mate = {"seq": seq + 1 - 2 * core}
    partner = {"chan": 1 - chan}
    above = {"seq": lax.rem(seq + 2, 2 * chips)}
    below = {"seq": lax.rem(seq + 2 * chips - 2, 2 * chips)}
    has_above = chip < chips - 1
    conv = lax.axis_index("dp")
    row = 2 * chan + lax.rem(conv, 2)
    col = lax.div(conv, 2)
    rows, cols = (4, convs // 2) if convs > 1 else (2, 1)
    row_step = 1 if convs > 1 else 2

    def chip_peer(k):
        there = lax.rem(chip + k, chips)
        return there, {"seq": 2 * there + core}

    def row_peer(k):
        there = lax.rem(row + k * row_step, 4)
        return there, {"chan": lax.div(there, 2), "dp": conv - lax.rem(conv, 2) + lax.rem(there, 2)}

    def col_peer(k):
        there = lax.rem(col + k, cols)
        return there, {"dp": 2 * there + lax.rem(conv, 2)}

    groups = (
        (bias_seq, seq_s, seq_r, chip, chip_peer, chips),
        (bias_row, row_s, row_r, row, row_peer, rows),
        (bias_col, col_s, col_r, col, col_peer, cols),
    )

    def remote(src, dst, send, recv, where):
        return pltpu.make_async_remote_copy(
            src_ref=src, dst_ref=dst, send_sem=send, recv_sem=recv, device_id=where, device_id_type=MESH
        )

    def loads(j):
        cols = pl.ds(pl.multiple_of(j * BLOCK, BLOCK), BLOCK)
        own = pl.ds(0, BLOCK)
        return (
            pltpu.make_async_copy(k_hbm.at[0, 0, :, cols], kv.at[0, j, 0], load_sem.at[0, j]),
            pltpu.make_async_copy(v_hbm.at[0, 0, :, cols], kv.at[0, j, 1], load_sem.at[1, j]),
            pltpu.make_async_copy(q_hbm.at[0, 0, :, cols], qg.at[j, 0, own], load_sem.at[2, j]),
            pltpu.make_async_copy(g_hbm.at[0, 0, :, cols], qg.at[j, 1, own], load_sem.at[3, j]),
        )

    def stores(j):
        cols = pl.ds(pl.multiple_of(j * BLOCK, BLOCK), BLOCK)
        return (
            pltpu.make_async_copy(out_stage.at[j, 0], dk_hbm.at[0, 0, :, cols], store_sem.at[0, j]),
            pltpu.make_async_copy(out_stage.at[j, 1], dv_hbm.at[0, 0, :, cols], store_sem.at[1, j]),
        )

    def store_query(j):
        cols = pl.ds(pl.multiple_of(j * BLOCK, BLOCK), BLOCK)
        return pltpu.make_async_copy(dq_stage.at[j], dq_hbm.at[0, 0, :, cols], store_sem.at[2, j])

    def hop(n, j):
        return remote(kv.at[2 * n - 2, j], kv.at[2 * n, j], hop_s.at[n - 1, j], hop_r.at[n - 1, j], above)

    def side(n, j):
        i = n - core
        return remote(kv.at[2 * n, j], kv.at[2 * i + 1, j], side_s.at[i, j], side_r.at[i, j], mate)

    def side_arrival(i, j):
        return remote(kv.at[2 * i + 1, j], kv.at[2 * i + 1, j], side_s.at[i, j], side_r.at[i, j], mate)

    def swap(j):
        return remote(
            qg.at[j, :, pl.ds(0, BLOCK)], qg.at[j, :, pl.ds(BLOCK, BLOCK)], swap_s.at[j], swap_r.at[j], partner
        )

    def stat(j):
        return remote(stat_out.at[j], stat_in.at[j], stat_s.at[j], stat_r.at[j], partner)

    def term(i, j):
        h = i + 1 - core
        return remote(side_out.at[i, j], side_in.at[h, j], term_s.at[i, j], term_r.at[h, j], mate)

    def term_arrival(h, j):
        return remote(side_in.at[h, j], side_in.at[h, j], term_s.at[0, j], term_r.at[h, j], mate)

    def chain(h, j):
        return remote(
            chain_out.at[h - 1, j], chain_in.at[h - 1, j], chain_s.at[h - 1, j], chain_r.at[h - 1, j], below
        )

    def query(j):
        return remote(dq_send.at[j], dq_recv.at[j], dq_s.at[j], dq_r.at[j], partner)

    def fetch(j, _):
        for copy in loads(j):
            copy.start()
        return 0

    lax.fori_loop(0, heads, fetch, 0)

    barrier = pltpu.get_barrier_semaphore()
    pl.semaphore_signal(barrier, inc=1, device_id=mate, device_id_type=MESH)
    for *_, peer, size in groups:
        for k in range(1, size):
            pl.semaphore_signal(barrier, inc=1, device_id=peer(k)[1], device_id_type=MESH)

    key_row = lax.broadcasted_iota(jnp.int32, (BLOCK, 2 * BLOCK), 0)
    query_col = lax.rem(lax.broadcasted_iota(jnp.int32, (BLOCK, 2 * BLOCK), 1), BLOCK)
    absent = [jnp.where(seq >= d, 0.0, NEG_FILL).astype(F32) for d in range(WINDOW)]
    tri[0] = jnp.where(key_row <= query_col, 0.0, NEG_FILL)
    tri[1] = jnp.where(key_row > query_col, 0.0, NEG_FILL) + absent[WINDOW - 1]
    lane = lax.rem(lax.broadcasted_iota(jnp.int32, (1, 2 * BLOCK), 1), BLOCK)
    valid = jnp.where(seq * BLOCK + lane < lengths[0], 1.0, 0.0).astype(F32)
    crossed = lax.broadcasted_iota(jnp.int32, (1, 2 * BLOCK), 1) >= BLOCK

    def clear(j, _):
        nothing = jnp.zeros((2, BLOCK, BLOCK), BF)
        for d in range(1, WINDOW):

            @pl.when(seq < d)
            def _():
                kv[d, j] = nothing

        @pl.when(core == 0)
        def _():
            side_in[3, j] = nothing

        @pl.when(core == 1)
        def _():
            side_in[0, j] = nothing

        @pl.when(jnp.logical_not(has_above))
        def _():
            for h in range(3):
                chain_in[h, j] = nothing

        return 0

    lax.fori_loop(0, heads, clear, 0)

    pl.semaphore_wait(barrier, chips + rows + cols - 2)

    def forward(j):
        swap(j).wait_recv()
        for i in range(3):

            @pl.when(seq >= 2 * i + 1)
            def _():
                side_arrival(i, j).wait_recv()

        queries, grads = qg[j, 0], qg[j, 1]
        peak = None
        for d in range(WINDOW):
            score = dot(kv[d, j, 0], queries, NT) * root_scale
            if d == 0:
                score = score + tri[0]
            elif d == WINDOW - 1:
                score = score + tri[1]
            else:
                score = score + absent[d]
            prob[d] = score
            top = jnp.max(score, axis=0, keepdims=True)
            peak = top if peak is None else jnp.maximum(peak, top)
        total = moment = None
        for d in range(WINDOW):
            weight_grad = dot(kv[d, j, 1], grads, NT)
            weight = jnp.exp(prob[d] - peak)
            prob[d] = weight
            wgrad[d] = weight_grad
            a = jnp.sum(weight, axis=0, keepdims=True)
            b = jnp.sum(weight * weight_grad, axis=0, keepdims=True)
            total = a if total is None else total + a
            moment = b if moment is None else moment + b
        offset = jnp.where(crossed, bias[j], 0.0)
        stat_out[j, 0:1] = peak + offset
        stat_out[j, 1:2] = total
        stat_out[j, 2:3] = moment
        stat_out[j, 3:8] = jnp.zeros((5, 2 * BLOCK), F32)
        stat(j).start()

    def backward(j):
        stat(j).wait_recv()

        def turned(row):
            theirs = stat_in[j, row : row + 1]
            return jnp.concatenate([theirs[:, BLOCK:], theirs[:, :BLOCK]], axis=1)

        peak = stat_out[j, 0:1]
        their_peak = turned(0)
        merged = jnp.maximum(peak, their_peak)
        mine, theirs = jnp.exp(peak - merged), jnp.exp(their_peak - merged)
        own_total = stat_out[j, 1:2] * mine
        own_moment = stat_out[j, 2:3] * mine
        inverse = valid / (own_total + turned(1) * theirs)
        delta = (own_moment + turned(2) * theirs) * inverse
        rescale = mine * inverse
        offset_term = (own_moment - delta * own_total) * inverse
        bias_out[pl.ds(j, 1), :] = offset_term[:, BLOCK:]

        @pl.when(j == heads - 1)
        def _():
            bias_out[...] = jnp.broadcast_to(jnp.sum(bias_out[...], axis=1, keepdims=True), bias_out.shape)
            mate_total().start()

        queries, grads = qg[j, 0], qg[j, 1]
        query_term = None
        for d in range(WINDOW):
            weight = prob[d] * rescale
            score_grad = (weight * (wgrad[d] - delta)).astype(BF)
            weight = weight.astype(BF)
            value_term = dot(weight, grads, NN)
            key_term = dot(score_grad, queries, NN) * root_scale
            part = dot(score_grad, kv[d, j, 0], TN)
            query_term = part if query_term is None else query_term + part
            if d % 2 == 0:
                terms[d // 2, j, 0] = key_term
                terms[d // 2, j, 1] = value_term
            else:
                side_out[d // 2, j, 0] = key_term.astype(BF)
                side_out[d // 2, j, 1] = value_term.astype(BF)
        query_term = query_term * root_scale
        dq_own[j] = query_term[:BLOCK]
        dq_send[j] = query_term[BLOCK:].astype(BF)
        for i in range(3):

            @pl.when(seq >= 2 * i + 1)
            def _():
                term(i, j).start()

        query(j).start()

    def mate_total():
        return remote(bias_out, bias_mate, mate_sem.at[0], mate_sem.at[1], mate)

    def spread(group):
        ref, send, recv, mine, peer, size = groups[group]
        for k in range(1, size):
            remote(ref.at[mine], ref.at[mine], send.at[k], recv.at[mine], peer(k)[1]).start()

    def gather(group):
        ref, send, recv, mine, peer, size = groups[group]
        for k in range(1, size):
            there, where = peer(k)
            remote(ref.at[there], ref.at[there], send.at[k], recv.at[there], where).wait_recv()
        slots = [ref[n * row_step if group == 1 else n] for n in range(size)]
        return functools.reduce(jnp.add, slots)

    def bias_stage(n):
        if n == 0:
            mate_total().wait_recv()
            bias_seq[chip] = bias_out[...] + bias_mate[...]
            spread(0)
        elif n == 1:
            bias_row[row] = gather(0)
            spread(1)
        elif n == 2:
            bias_col[col] = gather(1)
            spread(2)
        else:
            bias_mate[...] = gather(2)

    def within(j, action):
        @pl.when(jnp.logical_and(j >= 0, j < heads))
        def _():
            action(j)

    def send_own(j):
        for copy in loads(j):
            copy.wait()

        @pl.when(has_above)
        def _():
            hop(1, j).start()

        @pl.when(core == 0)
        def _():
            side(0, j).start()

        swap(j).start()

    def relay(n, j):
        @pl.when(chip >= n)
        def _():
            hop(n, j).wait_recv()
            if n < 3:

                @pl.when(has_above)
                def _():
                    hop(n + 1, j).start()

                side(n, j).start()
            else:

                @pl.when(core == 1)
                def _():
                    side(n, j).start()

    def finish_query(j):
        query(j).wait_recv()
        dq_stage[j] = (dq_own[j] + dq_recv[j].astype(F32)).astype(BF)
        store_query(j).start()

    def reduce(h, j):
        @pl.when(chip >= h)
        def _():
            if h == 3:
                pl.when(core == 1)(lambda: term_arrival(h, j).wait_recv())
            elif h == 0:
                pl.when(core == 0)(lambda: term_arrival(h, j).wait_recv())
            else:
                term_arrival(h, j).wait_recv()
            total = terms[h, j] + side_in[h, j].astype(F32)
            if h < 3:
                pl.when(has_above)(lambda: chain(h + 1, j).wait_recv())
                total = total + chain_in[h, j].astype(F32)
            if h > 0:
                chain_out[h - 1, j] = total.astype(BF)
                chain(h, j).start()
            else:
                out_stage[j] = total.astype(BF)
                for copy in stores(j):
                    copy.start()

    def step(i, _):
        within(i + 3, send_own)
        within(i + 2, functools.partial(relay, 1))
        within(i + 1, functools.partial(relay, 2))
        within(i, functools.partial(relay, 3))
        within(i - 1, backward)
        within(i, forward)
        within(i - 2, functools.partial(reduce, 3))
        within(i - 3, functools.partial(reduce, 2))
        within(i - 4, functools.partial(reduce, 1))
        within(i - 5, functools.partial(reduce, 0))
        within(i - 2, finish_query)
        for n in range(4):
            pl.when(i == heads + 1 + n)(functools.partial(bias_stage, n))
        return 0

    lax.fori_loop(-3, heads + 5, step, 0)

    def drain(j, _):
        swap(j).wait_send()
        stat(j).wait_send()
        query(j).wait_send()
        store_query(j).wait()
        for copy in stores(j):
            copy.wait()
        for n in range(1, 4):
            pl.when(jnp.logical_and(has_above, chip >= n - 1))(lambda: hop(n, j).wait_send())
        pl.when(core == 0)(lambda: side(0, j).wait_send())
        for n in (1, 2):
            pl.when(chip >= n)(lambda: side(n, j).wait_send())
        pl.when(jnp.logical_and(chip >= 3, core == 1))(lambda: side(3, j).wait_send())
        for i in range(3):
            pl.when(seq >= 2 * i + 1)(lambda: term(i, j).wait_send())
        for h in range(1, 4):
            pl.when(chip >= h)(lambda: chain(h, j).wait_send())
        return 0

    lax.fori_loop(0, heads, drain, 0)
    mate_total().wait_send()
    for ref, send, recv, mine, peer, size in groups:
        for k in range(1, size):
            remote(ref.at[mine], ref.at[mine], send.at[k], recv.at[mine], peer(k)[1]).wait_send()
    bias_out[...] = bias_mate[...]


def shards(queries, keys, values, out_grad, cross_bias, lengths):
    heads = cross_bias.shape[0]
    chips, convs = lax.axis_size("seq") // 2, lax.axis_size("dp")
    like = jax.ShapeDtypeStruct(queries.shape, BF)
    dma = pltpu.SemaphoreType.DMA
    anywhere = pl.BlockSpec(memory_space=pl.ANY)
    scalar = pl.BlockSpec(memory_space=pltpu.SMEM)
    tile = (BLOCK, BLOCK)
    wide = (BLOCK, 2 * BLOCK)
    query_grad, key_grad, value_grad, bias_rows = pl.pallas_call(
        functools.partial(kernel, heads, chips, convs),
        out_shape=(like, like, like, jax.ShapeDtypeStruct((heads, BLOCK), F32)),
        in_specs=[scalar, scalar] + [anywhere] * 4,
        out_specs=(anywhere, anywhere, anywhere, pl.BlockSpec(memory_space=pltpu.VMEM)),
        scratch_shapes=[
            pltpu.VMEM((WINDOW, heads, 2, *tile), BF),
            pltpu.VMEM((heads, 2, 2 * BLOCK, BLOCK), BF),
            pltpu.VMEM((2, *wide), F32),
            pltpu.VMEM((WINDOW, *wide), F32),
            pltpu.VMEM((WINDOW, *wide), F32),
            pltpu.VMEM((4, heads, 2, *tile), F32),
            pltpu.VMEM((3, heads, 2, *tile), BF),
            pltpu.VMEM((4, heads, 2, *tile), BF),
            pltpu.VMEM((3, heads, 2, *tile), BF),
            pltpu.VMEM((3, heads, 2, *tile), BF),
            pltpu.VMEM((heads, *tile), F32),
            pltpu.VMEM((heads, *tile), BF),
            pltpu.VMEM((heads, *tile), BF),
            pltpu.VMEM((heads, *tile), BF),
            pltpu.VMEM((heads, 2, *tile), BF),
            pltpu.VMEM((heads, 8, 2 * BLOCK), F32),
            pltpu.VMEM((heads, 8, 2 * BLOCK), F32),
            pltpu.VMEM((heads, BLOCK), F32),
            pltpu.VMEM((chips, heads, BLOCK), F32),
            pltpu.VMEM((4, heads, BLOCK), F32),
            pltpu.VMEM((4, heads, BLOCK), F32),
            dma((4, heads)),
            dma((3, heads)),
            dma((3, heads)),
            dma((3, heads)),
            dma((3, heads)),
            dma((heads,)),
            dma((heads,)),
            dma((heads,)),
            dma((heads,)),
            dma((3, heads)),
            dma((4, heads)),
            dma((3, heads)),
            dma((3, heads)),
            dma((heads,)),
            dma((heads,)),
            dma((3, heads)),
            dma((2,)),
            dma((chips,)),
            dma((chips,)),
            dma((4,)),
            dma((4,)),
            dma((4,)),
            dma((4,)),
        ],
        compiler_params=pltpu.CompilerParams(
            collective_id=0, has_side_effects=True, vmem_limit_bytes=56 * 1024 * 1024
        ),
    )(lengths, cross_bias, queries, keys, values, out_grad)
    return query_grad, key_grad, value_grad, bias_rows[:, 0]


def solution(mesh):
    split = P("dp", "chan", "seq", None)
    return jax.shard_map(
        shards,
        mesh=mesh,
        in_specs=(split, split, split, split, P(), P("dp")),
        out_specs=(split, split, split, P()),
        check_vma=False,
    )
```

```python
import functools
import math

import jax
import jax.numpy as jnp
from jax import lax
from jax.experimental import pallas as pl
from jax.experimental.pallas import tpu as pltpu
from jax.sharding import PartitionSpec as P

BLOCK = 128
WINDOW = 7
NEG_FILL = -1e30
MESH = pl.DeviceIdType.MESH
NT = (((1,), (1,)), ((), ()))
NN = (((1,), (0,)), ((), ()))
TN = (((0,), (0,)), ((), ()))
BF = jnp.bfloat16
F32 = jnp.float32


def dot(a, b, dims):
    return lax.dot_general(a, b, dims, preferred_element_type=F32)


def kernel(
    heads,
    chips,
    convs,
    lengths,
    bias,
    q_hbm,
    k_hbm,
    v_hbm,
    g_hbm,
    dq_hbm,
    dk_hbm,
    dv_hbm,
    bias_out,
    kv,
    qg,
    tri,
    prob,
    wgrad,
    terms,
    side_out,
    side_in,
    chain_out,
    chain_in,
    dq_own,
    dq_send,
    dq_recv,
    dq_stage,
    out_stage,
    stat_out,
    stat_in,
    bias_mate,
    bias_seq,
    bias_row,
    bias_col,
    load_sem,
    hop_s,
    hop_r,
    side_s,
    side_r,
    swap_s,
    swap_r,
    stat_s,
    stat_r,
    term_s,
    term_r,
    chain_s,
    chain_r,
    dq_s,
    dq_r,
    store_sem,
    mate_sem,
    seq_s,
    seq_r,
    row_s,
    row_r,
    col_s,
    col_r,
):
    root_scale = 1.0 / math.sqrt(BLOCK)
    chan = lax.axis_index("chan")
    seq = lax.axis_index("seq")
    chip = lax.div(seq, 2)
    core = lax.rem(seq, 2)
    mate = {"seq": seq + 1 - 2 * core}
    partner = {"chan": 1 - chan}
    above = {"seq": lax.rem(seq + 2, 2 * chips)}
    below = {"seq": lax.rem(seq + 2 * chips - 2, 2 * chips)}
    has_above = chip < chips - 1
    conv = lax.axis_index("dp")
    row = 2 * chan + lax.rem(conv, 2)
    col = lax.div(conv, 2)
    rows, cols = (4, convs // 2) if convs > 1 else (2, 1)
    row_step = 1 if convs > 1 else 2

    def chip_peer(k):
        there = lax.rem(chip + k, chips)
        return there, {"seq": 2 * there + core}

    def row_peer(k):
        there = lax.rem(row + k * row_step, 4)
        return there, {"chan": lax.div(there, 2), "dp": conv - lax.rem(conv, 2) + lax.rem(there, 2)}

    def col_peer(k):
        there = lax.rem(col + k, cols)
        return there, {"dp": 2 * there + lax.rem(conv, 2)}

    groups = (
        (bias_seq, seq_s, seq_r, chip, chip_peer, chips),
        (bias_row, row_s, row_r, row, row_peer, rows),
        (bias_col, col_s, col_r, col, col_peer, cols),
    )

    def remote(src, dst, send, recv, where):
        return pltpu.make_async_remote_copy(
            src_ref=src, dst_ref=dst, send_sem=send, recv_sem=recv, device_id=where, device_id_type=MESH
        )

    def loads(j):
        cols = pl.ds(pl.multiple_of(j * BLOCK, BLOCK), BLOCK)
        own = pl.ds(0, BLOCK)
        return (
            pltpu.make_async_copy(k_hbm.at[0, 0, :, cols], kv.at[0, j, 0], load_sem.at[0, j]),
            pltpu.make_async_copy(v_hbm.at[0, 0, :, cols], kv.at[0, j, 1], load_sem.at[1, j]),
            pltpu.make_async_copy(q_hbm.at[0, 0, :, cols], qg.at[j, 0, own], load_sem.at[2, j]),
            pltpu.make_async_copy(g_hbm.at[0, 0, :, cols], qg.at[j, 1, own], load_sem.at[3, j]),
        )

    def stores(j):
        cols = pl.ds(pl.multiple_of(j * BLOCK, BLOCK), BLOCK)
        return (
            pltpu.make_async_copy(out_stage.at[j, 0], dk_hbm.at[0, 0, :, cols], store_sem.at[0, j]),
            pltpu.make_async_copy(out_stage.at[j, 1], dv_hbm.at[0, 0, :, cols], store_sem.at[1, j]),
        )

    def store_query(j):
        cols = pl.ds(pl.multiple_of(j * BLOCK, BLOCK), BLOCK)
        return pltpu.make_async_copy(dq_stage.at[j], dq_hbm.at[0, 0, :, cols], store_sem.at[2, j])

    def hop(n, j):
        return remote(kv.at[2 * n - 2, j], kv.at[2 * n, j], hop_s.at[n - 1, j], hop_r.at[n - 1, j], above)

    def side(n, j):
        i = n - core
        return remote(kv.at[2 * n, j], kv.at[2 * i + 1, j], side_s.at[i, j], side_r.at[i, j], mate)

    def side_arrival(i, j):
        return remote(kv.at[2 * i + 1, j], kv.at[2 * i + 1, j], side_s.at[i, j], side_r.at[i, j], mate)

    def swap(j):
        return remote(
            qg.at[j, :, pl.ds(0, BLOCK)], qg.at[j, :, pl.ds(BLOCK, BLOCK)], swap_s.at[j], swap_r.at[j], partner
        )

    def stat(j):
        return remote(stat_out.at[j], stat_in.at[j], stat_s.at[j], stat_r.at[j], partner)

    def term(i, j):
        h = i + 1 - core
        return remote(side_out.at[i, j], side_in.at[h, j], term_s.at[i, j], term_r.at[h, j], mate)

    def term_arrival(h, j):
        return remote(side_in.at[h, j], side_in.at[h, j], term_s.at[0, j], term_r.at[h, j], mate)

    def chain(h, j):
        return remote(
            chain_out.at[h - 1, j], chain_in.at[h - 1, j], chain_s.at[h - 1, j], chain_r.at[h - 1, j], below
        )

    def query(j):
        return remote(dq_send.at[j], dq_recv.at[j], dq_s.at[j], dq_r.at[j], partner)

    def fetch(j, _):
        for copy in loads(j):
            copy.start()
        return 0

    lax.fori_loop(0, heads, fetch, 0)

    barrier = pltpu.get_barrier_semaphore()
    pl.semaphore_signal(barrier, inc=1, device_id=mate, device_id_type=MESH)
    for *_, peer, size in groups:
        for k in range(1, size):
            pl.semaphore_signal(barrier, inc=1, device_id=peer(k)[1], device_id_type=MESH)

    key_row = lax.broadcasted_iota(jnp.int32, (BLOCK, 2 * BLOCK), 0)
    query_col = lax.rem(lax.broadcasted_iota(jnp.int32, (BLOCK, 2 * BLOCK), 1), BLOCK)
    absent = [jnp.where(seq >= d, 0.0, NEG_FILL).astype(F32) for d in range(WINDOW)]
    tri[0] = jnp.where(key_row <= query_col, 0.0, NEG_FILL)
    tri[1] = jnp.where(key_row > query_col, 0.0, NEG_FILL) + absent[WINDOW - 1]
    lane = lax.rem(lax.broadcasted_iota(jnp.int32, (1, 2 * BLOCK), 1), BLOCK)
    valid = jnp.where(seq * BLOCK + lane < lengths[0], 1.0, 0.0).astype(F32)
    crossed = lax.broadcasted_iota(jnp.int32, (1, 2 * BLOCK), 1) >= BLOCK

    def clear(j, _):
        nothing = jnp.zeros((2, BLOCK, BLOCK), BF)
        for d in range(1, WINDOW):

            @pl.when(seq < d)
            def _():
                kv[d, j] = nothing

        @pl.when(core == 0)
        def _():
            side_in[3, j] = nothing

        @pl.when(core == 1)
        def _():
            side_in[0, j] = nothing

        @pl.when(jnp.logical_not(has_above))
        def _():
            for h in range(3):
                chain_in[h, j] = nothing

        return 0

    lax.fori_loop(0, heads, clear, 0)

    pl.semaphore_wait(barrier, chips + rows + cols - 2)

    def forward(j):
        swap(j).wait_recv()
        for i in range(3):

            @pl.when(seq >= 2 * i + 1)
            def _():
                side_arrival(i, j).wait_recv()

        queries, grads = qg[j, 0], qg[j, 1]
        slot = lax.rem(j, 2)
        peak = None
        for d in range(WINDOW):
            score = dot(kv[d, j, 0], queries, NT) * root_scale
            if d == 0:
                score = score + tri[0]
            elif d == WINDOW - 1:
                score = score + tri[1]
            else:
                score = score + absent[d]
            prob[slot, d] = score
            top = jnp.max(score, axis=0, keepdims=True)
            peak = top if peak is None else jnp.maximum(peak, top)
        total = moment = None
        for d in range(WINDOW):
            weight_grad = dot(kv[d, j, 1], grads, NT)
            weight = jnp.exp(prob[slot, d] - peak)
            prob[slot, d] = weight
            wgrad[slot, d] = weight_grad
            a = jnp.sum(weight, axis=0, keepdims=True)
            b = jnp.sum(weight * weight_grad, axis=0, keepdims=True)
            total = a if total is None else total + a
            moment = b if moment is None else moment + b
        offset = jnp.where(crossed, bias[j], 0.0)
        stat_out[j, 0:1] = peak + offset
        stat_out[j, 1:2] = total
        stat_out[j, 2:3] = moment
        stat_out[j, 3:8] = jnp.zeros((5, 2 * BLOCK), F32)
        stat(j).start()

    def backward(j):
        stat(j).wait_recv()

        def turned(row):
            theirs = stat_in[j, row : row + 1]
            return jnp.concatenate([theirs[:, BLOCK:], theirs[:, :BLOCK]], axis=1)

        peak = stat_out[j, 0:1]
        their_peak = turned(0)
        merged = jnp.maximum(peak, their_peak)
        mine, theirs = jnp.exp(peak - merged), jnp.exp(their_peak - merged)
        own_total = stat_out[j, 1:2] * mine
        own_moment = stat_out[j, 2:3] * mine
        inverse = valid / (own_total + turned(1) * theirs)
        delta = (own_moment + turned(2) * theirs) * inverse
        rescale = mine * inverse
        offset_term = (own_moment - delta * own_total) * inverse
        bias_out[pl.ds(j, 1), :] = offset_term[:, BLOCK:]

        @pl.when(j == heads - 1)
        def _():
            bias_out[...] = jnp.broadcast_to(jnp.sum(bias_out[...], axis=1, keepdims=True), bias_out.shape)
            mate_total().start()

        queries, grads = qg[j, 0], qg[j, 1]
        slot = lax.rem(j, 2)
        query_term = None
        for d in range(WINDOW):
            weight = prob[slot, d] * rescale
            score_grad = (weight * (wgrad[slot, d] - delta)).astype(BF)
            weight = weight.astype(BF)
            value_term = dot(weight, grads, NN)
            key_term = dot(score_grad, queries, NN) * root_scale
            part = dot(score_grad, kv[d, j, 0], TN)
            query_term = part if query_term is None else query_term + part
            if d % 2 == 0:
                terms[d // 2, j, 0] = key_term
                terms[d // 2, j, 1] = value_term
            else:
                side_out[d // 2, j, 0] = key_term.astype(BF)
                side_out[d // 2, j, 1] = value_term.astype(BF)
        query_term = query_term * root_scale
        dq_own[j] = query_term[:BLOCK]
        dq_send[j] = query_term[BLOCK:].astype(BF)
        for i in range(3):

            @pl.when(seq >= 2 * i + 1)
            def _():
                term(i, j).start()

        query(j).start()

    def mate_total():
        return remote(bias_out, bias_mate, mate_sem.at[0], mate_sem.at[1], mate)

    def spread(group):
        ref, send, recv, mine, peer, size = groups[group]
        for k in range(1, size):
            remote(ref.at[mine], ref.at[mine], send.at[k], recv.at[mine], peer(k)[1]).start()

    def gather(group):
        ref, send, recv, mine, peer, size = groups[group]
        for k in range(1, size):
            there, where = peer(k)
            remote(ref.at[there], ref.at[there], send.at[k], recv.at[there], where).wait_recv()
        slots = [ref[n * row_step if group == 1 else n] for n in range(size)]
        return functools.reduce(jnp.add, slots)

    def bias_stage(n):
        if n == 0:
            mate_total().wait_recv()
            bias_seq[chip] = bias_out[...] + bias_mate[...]
            spread(0)
        elif n == 1:
            bias_row[row] = gather(0)
            spread(1)
        elif n == 2:
            bias_col[col] = gather(1)
            spread(2)
        else:
            bias_mate[...] = gather(2)

    def within(j, action):
        @pl.when(jnp.logical_and(j >= 0, j < heads))
        def _():
            action(j)

    def send_own(j):
        for copy in loads(j):
            copy.wait()

        @pl.when(has_above)
        def _():
            hop(1, j).start()

        @pl.when(core == 0)
        def _():
            side(0, j).start()

        swap(j).start()

    def relay(n, j):
        @pl.when(chip >= n)
        def _():
            hop(n, j).wait_recv()
            if n < 3:

                @pl.when(has_above)
                def _():
                    hop(n + 1, j).start()

                side(n, j).start()
            else:

                @pl.when(core == 1)
                def _():
                    side(n, j).start()

    def finish_query(j):
        query(j).wait_recv()
        dq_stage[j] = (dq_own[j] + dq_recv[j].astype(F32)).astype(BF)
        store_query(j).start()

    def reduce(h, j):
        @pl.when(chip >= h)
        def _():
            if h == 3:
                pl.when(core == 1)(lambda: term_arrival(h, j).wait_recv())
            elif h == 0:
                pl.when(core == 0)(lambda: term_arrival(h, j).wait_recv())
            else:
                term_arrival(h, j).wait_recv()
            total = terms[h, j] + side_in[h, j].astype(F32)
            if h < 3:
                pl.when(has_above)(lambda: chain(h + 1, j).wait_recv())
                total = total + chain_in[h, j].astype(F32)
            if h > 0:
                chain_out[h - 1, j] = total.astype(BF)
                chain(h, j).start()
            else:
                out_stage[j] = total.astype(BF)
                for copy in stores(j):
                    copy.start()

    def step(i, _):
        within(i + 2, functools.partial(relay, 1))
        within(i + 1, functools.partial(relay, 2))
        within(i + 4, send_own)
        within(i, functools.partial(relay, 3))
        within(i - 4, functools.partial(reduce, 2))
        within(i - 5, functools.partial(reduce, 1))
        within(i - 2, functools.partial(reduce, 3))
        within(i - 6, functools.partial(reduce, 0))
        within(i, forward)
        within(i - 1, backward)
        within(i - 3, finish_query)
        for n in range(4):
            pl.when(i == heads + 1 + 1 * n)(functools.partial(bias_stage, n))
        return 0

    lax.fori_loop(-4, heads + 6, step, 0)

    def drain(j, _):
        swap(j).wait_send()
        stat(j).wait_send()
        query(j).wait_send()
        store_query(j).wait()
        for copy in stores(j):
            copy.wait()
        for n in range(1, 4):
            pl.when(jnp.logical_and(has_above, chip >= n - 1))(lambda: hop(n, j).wait_send())
        pl.when(core == 0)(lambda: side(0, j).wait_send())
        for n in (1, 2):
            pl.when(chip >= n)(lambda: side(n, j).wait_send())
        pl.when(jnp.logical_and(chip >= 3, core == 1))(lambda: side(3, j).wait_send())
        for i in range(3):
            pl.when(seq >= 2 * i + 1)(lambda: term(i, j).wait_send())
        for h in range(1, 4):
            pl.when(chip >= h)(lambda: chain(h, j).wait_send())
        return 0

    lax.fori_loop(0, heads, drain, 0)
    mate_total().wait_send()
    for ref, send, recv, mine, peer, size in groups:
        for k in range(1, size):
            remote(ref.at[mine], ref.at[mine], send.at[k], recv.at[mine], peer(k)[1]).wait_send()
    bias_out[...] = bias_mate[...]


def shards(queries, keys, values, out_grad, cross_bias, lengths):
    heads = cross_bias.shape[0]
    chips, convs = lax.axis_size("seq") // 2, lax.axis_size("dp")
    like = jax.ShapeDtypeStruct(queries.shape, BF)
    dma = pltpu.SemaphoreType.DMA
    anywhere = pl.BlockSpec(memory_space=pl.ANY)
    scalar = pl.BlockSpec(memory_space=pltpu.SMEM)
    tile = (BLOCK, BLOCK)
    wide = (BLOCK, 2 * BLOCK)
    query_grad, key_grad, value_grad, bias_rows = pl.pallas_call(
        functools.partial(kernel, heads, chips, convs),
        out_shape=(like, like, like, jax.ShapeDtypeStruct((heads, BLOCK), F32)),
        in_specs=[scalar, scalar] + [anywhere] * 4,
        out_specs=(anywhere, anywhere, anywhere, pl.BlockSpec(memory_space=pltpu.VMEM)),
        scratch_shapes=[
            pltpu.VMEM((WINDOW, heads, 2, *tile), BF),
            pltpu.VMEM((heads, 2, 2 * BLOCK, BLOCK), BF),
            pltpu.VMEM((2, *wide), F32),
            pltpu.VMEM((2, WINDOW, *wide), F32),
            pltpu.VMEM((2, WINDOW, *wide), F32),
            pltpu.VMEM((4, heads, 2, *tile), F32),
            pltpu.VMEM((3, heads, 2, *tile), BF),
            pltpu.VMEM((4, heads, 2, *tile), BF),
            pltpu.VMEM((3, heads, 2, *tile), BF),
            pltpu.VMEM((3, heads, 2, *tile), BF),
            pltpu.VMEM((heads, *tile), F32),
            pltpu.VMEM((heads, *tile), BF),
            pltpu.VMEM((heads, *tile), BF),
            pltpu.VMEM((heads, *tile), BF),
            pltpu.VMEM((heads, 2, *tile), BF),
            pltpu.VMEM((heads, 8, 2 * BLOCK), F32),
            pltpu.VMEM((heads, 8, 2 * BLOCK), F32),
            pltpu.VMEM((heads, BLOCK), F32),
            pltpu.VMEM((chips, heads, BLOCK), F32),
            pltpu.VMEM((4, heads, BLOCK), F32),
            pltpu.VMEM((4, heads, BLOCK), F32),
            dma((4, heads)),
            dma((3, heads)),
            dma((3, heads)),
            dma((3, heads)),
            dma((3, heads)),
            dma((heads,)),
            dma((heads,)),
            dma((heads,)),
            dma((heads,)),
            dma((3, heads)),
            dma((4, heads)),
            dma((3, heads)),
            dma((3, heads)),
            dma((heads,)),
            dma((heads,)),
            dma((3, heads)),
            dma((2,)),
            dma((chips,)),
            dma((chips,)),
            dma((4,)),
            dma((4,)),
            dma((4,)),
            dma((4,)),
        ],
        compiler_params=pltpu.CompilerParams(
            collective_id=0, has_side_effects=True, vmem_limit_bytes=56 * 1024 * 1024
        ),
    )(lengths, cross_bias, queries, keys, values, out_grad)
    return query_grad, key_grad, value_grad, bias_rows[:, 0]


def solution(mesh):
    split = P("dp", "chan", "seq", None)
    return jax.shard_map(
        shards,
        mesh=mesh,
        in_specs=(split, split, split, split, P(), P("dp")),
        out_specs=(split, split, split, P()),
        check_vma=False,
    )
```

```python
import functools
import math

import jax
import jax.numpy as jnp
from jax import lax
from jax.experimental import pallas as pl
from jax.experimental.pallas import tpu as pltpu
from jax.sharding import PartitionSpec as P

BLOCK = 128
WINDOW = 7
NEG_FILL = -1e30
MESH = pl.DeviceIdType.MESH
NT = (((1,), (1,)), ((), ()))
NN = (((1,), (0,)), ((), ()))
TN = (((0,), (0,)), ((), ()))
BF = jnp.bfloat16
F32 = jnp.float32


def dot(a, b, dims):
    return lax.dot_general(a, b, dims, preferred_element_type=F32)


def kernel(
    heads,
    chips,
    convs,
    lengths,
    bias,
    q_hbm,
    k_hbm,
    v_hbm,
    g_hbm,
    dq_stage,
    out_stage,
    bias_final,
    kv,
    qg,
    tri,
    prob,
    wgrad,
    terms,
    side_out,
    side_in,
    chain_out,
    chain_in,
    dq_own,
    dq_send,
    dq_recv,
    stat_out,
    stat_in,
    bias_out,
    bias_mate,
    bias_seq,
    bias_row,
    bias_col,
    load_sem,
    hop_s,
    hop_r,
    side_s,
    side_r,
    swap_s,
    swap_r,
    stat_s,
    stat_r,
    term_s,
    term_r,
    chain_s,
    chain_r,
    dq_s,
    dq_r,
    mate_sem,
    seq_s,
    seq_r,
    row_s,
    row_r,
    col_s,
    col_r,
):
    root_scale = 1.0 / math.sqrt(BLOCK)
    chan = lax.axis_index("chan")
    seq = lax.axis_index("seq")
    chip = lax.div(seq, 2)
    core = lax.rem(seq, 2)
    mate = {"seq": seq + 1 - 2 * core}
    partner = {"chan": 1 - chan}
    above = {"seq": lax.rem(seq + 2, 2 * chips)}
    below = {"seq": lax.rem(seq + 2 * chips - 2, 2 * chips)}
    has_above = chip < chips - 1
    conv = lax.axis_index("dp")
    row = 2 * chan + lax.rem(conv, 2)
    col = lax.div(conv, 2)
    rows, cols = (4, convs // 2) if convs > 1 else (2, 1)
    row_step = 1 if convs > 1 else 2

    def chip_peer(k):
        there = lax.rem(chip + k, chips)
        return there, {"seq": 2 * there + core}

    def row_peer(k):
        there = lax.rem(row + k * row_step, 4)
        return there, {"chan": lax.div(there, 2), "dp": conv - lax.rem(conv, 2) + lax.rem(there, 2)}

    def col_peer(k):
        there = lax.rem(col + k, cols)
        return there, {"dp": 2 * there + lax.rem(conv, 2)}

    groups = (
        (bias_seq, seq_s, seq_r, chip, chip_peer, chips),
        (bias_row, row_s, row_r, row, row_peer, rows),
        (bias_col, col_s, col_r, col, col_peer, cols),
    )

    def remote(src, dst, send, recv, where):
        return pltpu.make_async_remote_copy(
            src_ref=src, dst_ref=dst, send_sem=send, recv_sem=recv, device_id=where, device_id_type=MESH
        )

    def loads(j):
        cols = pl.ds(pl.multiple_of(j * BLOCK, BLOCK), BLOCK)
        own = pl.ds(0, BLOCK)
        return (
            pltpu.make_async_copy(k_hbm.at[0, 0, :, cols], kv.at[0, j, 0], load_sem.at[0, j]),
            pltpu.make_async_copy(v_hbm.at[0, 0, :, cols], kv.at[0, j, 1], load_sem.at[1, j]),
            pltpu.make_async_copy(q_hbm.at[0, 0, :, cols], qg.at[j, 0, own], load_sem.at[2, j]),
            pltpu.make_async_copy(g_hbm.at[0, 0, :, cols], qg.at[j, 1, own], load_sem.at[3, j]),
        )

    def hop(n, j):
        return remote(kv.at[2 * n - 2, j], kv.at[2 * n, j], hop_s.at[n - 1, j], hop_r.at[n - 1, j], above)

    def side(n, j):
        i = n - core
        return remote(kv.at[2 * n, j], kv.at[2 * i + 1, j], side_s.at[i, j], side_r.at[i, j], mate)

    def side_arrival(i, j):
        return remote(kv.at[2 * i + 1, j], kv.at[2 * i + 1, j], side_s.at[i, j], side_r.at[i, j], mate)

    def swap(j):
        return remote(
            qg.at[j, :, pl.ds(0, BLOCK)], qg.at[j, :, pl.ds(BLOCK, BLOCK)], swap_s.at[j], swap_r.at[j], partner
        )

    def stat(j):
        return remote(stat_out.at[j], stat_in.at[j], stat_s.at[j], stat_r.at[j], partner)

    def term(i, j):
        h = i + 1 - core
        return remote(side_out.at[i, j], side_in.at[h, j], term_s.at[i, j], term_r.at[h, j], mate)

    def term_arrival(h, j):
        return remote(side_in.at[h, j], side_in.at[h, j], term_s.at[0, j], term_r.at[h, j], mate)

    def chain(h, j):
        return remote(
            chain_out.at[h - 1, j], chain_in.at[h - 1, j], chain_s.at[h - 1, j], chain_r.at[h - 1, j], below
        )

    def query(j):
        return remote(dq_send.at[j], dq_recv.at[j], dq_s.at[j], dq_r.at[j], partner)

    def fetch(j, _):
        for copy in loads(j):
            copy.start()
        return 0

    lax.fori_loop(0, heads, fetch, 0)

    barrier = pltpu.get_barrier_semaphore()
    pl.semaphore_signal(barrier, inc=1, device_id=mate, device_id_type=MESH)
    for *_, peer, size in groups:
        for k in range(1, size):
            pl.semaphore_signal(barrier, inc=1, device_id=peer(k)[1], device_id_type=MESH)

    key_row = lax.broadcasted_iota(jnp.int32, (BLOCK, 2 * BLOCK), 0)
    query_col = lax.rem(lax.broadcasted_iota(jnp.int32, (BLOCK, 2 * BLOCK), 1), BLOCK)
    absent = [jnp.where(seq >= d, 0.0, NEG_FILL).astype(F32) for d in range(WINDOW)]
    tri[0] = jnp.where(key_row <= query_col, 0.0, NEG_FILL)
    tri[1] = jnp.where(key_row > query_col, 0.0, NEG_FILL) + absent[WINDOW - 1]
    lane = lax.rem(lax.broadcasted_iota(jnp.int32, (1, 2 * BLOCK), 1), BLOCK)
    valid = jnp.where(seq * BLOCK + lane < lengths[0], 1.0, 0.0).astype(F32)
    crossed = lax.broadcasted_iota(jnp.int32, (1, 2 * BLOCK), 1) >= BLOCK

    def clear(j, _):
        nothing = jnp.zeros((2, BLOCK, BLOCK), BF)
        for d in range(1, WINDOW):

            @pl.when(seq < d)
            def _():
                kv[d, j] = nothing

        @pl.when(core == 0)
        def _():
            side_in[3, j] = nothing

        @pl.when(core == 1)
        def _():
            side_in[0, j] = nothing

        @pl.when(jnp.logical_not(has_above))
        def _():
            for h in range(3):
                chain_in[h, j] = nothing

        return 0

    lax.fori_loop(0, heads, clear, 0)

    pl.semaphore_wait(barrier, chips + rows + cols - 2)

    def forward(j):
        swap(j).wait_recv()
        for i in range(3):

            @pl.when(seq >= 2 * i + 1)
            def _():
                side_arrival(i, j).wait_recv()

        queries, grads = qg[j, 0], qg[j, 1]
        slot = lax.rem(j, 2)
        peak = None
        for d in range(WINDOW):
            score = dot(kv[d, j, 0], queries, NT) * root_scale
            if d == 0:
                score = score + tri[0]
            elif d == WINDOW - 1:
                score = score + tri[1]
            else:
                score = score + absent[d]
            prob[slot, d] = score
            top = jnp.max(score, axis=0, keepdims=True)
            peak = top if peak is None else jnp.maximum(peak, top)
        total = moment = None
        for d in range(WINDOW):
            weight_grad = dot(kv[d, j, 1], grads, NT)
            weight = jnp.exp(prob[slot, d] - peak)
            prob[slot, d] = weight
            wgrad[slot, d] = weight_grad
            a = jnp.sum(weight, axis=0, keepdims=True)
            b = jnp.sum(weight * weight_grad, axis=0, keepdims=True)
            total = a if total is None else total + a
            moment = b if moment is None else moment + b
        offset = jnp.where(crossed, bias[j], 0.0)
        stat_out[j, 0:1] = peak + offset
        stat_out[j, 1:2] = total
        stat_out[j, 2:3] = moment
        stat_out[j, 3:8] = jnp.zeros((5, 2 * BLOCK), F32)
        stat(j).start()

    def backward(j):
        stat(j).wait_recv()

        def turned(row):
            theirs = stat_in[j, row : row + 1]
            return jnp.concatenate([theirs[:, BLOCK:], theirs[:, :BLOCK]], axis=1)

        peak = stat_out[j, 0:1]
        their_peak = turned(0)
        merged = jnp.maximum(peak, their_peak)
        mine, theirs = jnp.exp(peak - merged), jnp.exp(their_peak - merged)
        own_total = stat_out[j, 1:2] * mine
        own_moment = stat_out[j, 2:3] * mine
        inverse = valid / (own_total + turned(1) * theirs)
        delta = (own_moment + turned(2) * theirs) * inverse
        rescale = mine * inverse
        offset_term = (own_moment - delta * own_total) * inverse
        bias_out[pl.ds(j, 1), :] = offset_term[:, BLOCK:]

        @pl.when(j == heads - 1)
        def _():
            bias_out[...] = jnp.broadcast_to(jnp.sum(bias_out[...], axis=1, keepdims=True), bias_out.shape)
            mate_total().start()

        queries, grads = qg[j, 0], qg[j, 1]
        slot = lax.rem(j, 2)
        query_term = None
        for d in range(WINDOW):
            weight = prob[slot, d] * rescale
            score_grad = (weight * (wgrad[slot, d] - delta)).astype(BF)
            weight = weight.astype(BF)
            value_term = dot(weight, grads, NN)
            key_term = dot(score_grad, queries, NN) * root_scale
            part = dot(score_grad, kv[d, j, 0], TN)
            query_term = part if query_term is None else query_term + part
            if d % 2 == 0:
                terms[d // 2, j, 0] = key_term
                terms[d // 2, j, 1] = value_term
            else:
                side_out[d // 2, j, 0] = key_term.astype(BF)
                side_out[d // 2, j, 1] = value_term.astype(BF)
        query_term = query_term * root_scale
        dq_own[j] = query_term[:BLOCK]
        dq_send[j] = query_term[BLOCK:].astype(BF)
        for i in range(3):

            @pl.when(seq >= 2 * i + 1)
            def _():
                term(i, j).start()

        query(j).start()

    def mate_total():
        return remote(bias_out, bias_mate, mate_sem.at[0], mate_sem.at[1], mate)

    def spread(group):
        ref, send, recv, mine, peer, size = groups[group]
        for k in range(1, size):
            remote(ref.at[mine], ref.at[mine], send.at[k], recv.at[mine], peer(k)[1]).start()

    def gather(group):
        ref, send, recv, mine, peer, size = groups[group]
        for k in range(1, size):
            there, where = peer(k)
            remote(ref.at[there], ref.at[there], send.at[k], recv.at[there], where).wait_recv()
        slots = [ref[n * row_step if group == 1 else n] for n in range(size)]
        return functools.reduce(jnp.add, slots)

    def bias_stage(n):
        if n == 0:
            mate_total().wait_recv()
            bias_seq[chip] = bias_out[...] + bias_mate[...]
            spread(0)
        elif n == 1:
            bias_row[row] = gather(0)
            spread(1)
        elif n == 2:
            bias_col[col] = gather(1)
            spread(2)
        else:
            bias_mate[...] = gather(2)

    def within(j, action):
        @pl.when(jnp.logical_and(j >= 0, j < heads))
        def _():
            action(j)

    def send_own(j):
        for copy in loads(j):
            copy.wait()

        @pl.when(has_above)
        def _():
            hop(1, j).start()

        @pl.when(core == 0)
        def _():
            side(0, j).start()

        swap(j).start()

    def relay(n, j):
        @pl.when(chip >= n)
        def _():
            hop(n, j).wait_recv()
            if n < 3:

                @pl.when(has_above)
                def _():
                    hop(n + 1, j).start()

                side(n, j).start()
            else:

                @pl.when(core == 1)
                def _():
                    side(n, j).start()

    def finish_query(j):
        query(j).wait_recv()
        dq_stage[j] = (dq_own[j] + dq_recv[j].astype(F32)).astype(BF)

    def reduce(h, j):
        @pl.when(chip >= h)
        def _():
            if h == 3:
                pl.when(core == 1)(lambda: term_arrival(h, j).wait_recv())
            elif h == 0:
                pl.when(core == 0)(lambda: term_arrival(h, j).wait_recv())
            else:
                term_arrival(h, j).wait_recv()
            total = terms[h, j] + side_in[h, j].astype(F32)
            if h < 3:
                pl.when(has_above)(lambda: chain(h + 1, j).wait_recv())
                total = total + chain_in[h, j].astype(F32)
            if h > 0:
                chain_out[h - 1, j] = total.astype(BF)
                chain(h, j).start()
            else:
                out_stage[j] = total.astype(BF)

    def step(i, _):
        within(i + 2, functools.partial(relay, 1))
        within(i + 1, functools.partial(relay, 2))
        within(i + 4, send_own)
        within(i, functools.partial(relay, 3))
        within(i - 4, functools.partial(reduce, 2))
        within(i - 5, functools.partial(reduce, 1))
        within(i - 2, functools.partial(reduce, 3))
        within(i - 6, functools.partial(reduce, 0))
        within(i, forward)
        within(i - 1, backward)
        within(i - 3, finish_query)
        for n in range(4):
            pl.when(i == heads + 1 + 1 * n)(functools.partial(bias_stage, n))
        return 0

    lax.fori_loop(-4, heads + 6, step, 0)

    def drain(j, _):
        swap(j).wait_send()
        stat(j).wait_send()
        query(j).wait_send()
        for n in range(1, 4):
            pl.when(jnp.logical_and(has_above, chip >= n - 1))(lambda: hop(n, j).wait_send())
        pl.when(core == 0)(lambda: side(0, j).wait_send())
        for n in (1, 2):
            pl.when(chip >= n)(lambda: side(n, j).wait_send())
        pl.when(jnp.logical_and(chip >= 3, core == 1))(lambda: side(3, j).wait_send())
        for i in range(3):
            pl.when(seq >= 2 * i + 1)(lambda: term(i, j).wait_send())
        for h in range(1, 4):
            pl.when(chip >= h)(lambda: chain(h, j).wait_send())
        return 0

    lax.fori_loop(0, heads, drain, 0)
    mate_total().wait_send()
    for ref, send, recv, mine, peer, size in groups:
        for k in range(1, size):
            remote(ref.at[mine], ref.at[mine], send.at[k], recv.at[mine], peer(k)[1]).wait_send()
    head_row = lax.broadcasted_iota(jnp.int32, (heads, BLOCK), 0)
    head_lane = lax.broadcasted_iota(jnp.int32, (heads, BLOCK), 1)
    picked = jnp.where(head_row == head_lane, bias_mate[...], 0.0)
    bias_final[...] = jnp.sum(picked, axis=0, keepdims=True)


def publish(heads, dq_stage, out_stage, bias_final, dq_hbm, dk_hbm, dv_hbm, bias_out, sem):
    def copies(j):
        cols = pl.ds(pl.multiple_of(j * BLOCK, BLOCK), BLOCK)
        return (
            pltpu.make_async_copy(dq_stage.at[j], dq_hbm.at[0, 0, :, cols], sem.at[0, j]),
            pltpu.make_async_copy(out_stage.at[j, 0], dk_hbm.at[0, 0, :, cols], sem.at[1, j]),
            pltpu.make_async_copy(out_stage.at[j, 1], dv_hbm.at[0, 0, :, cols], sem.at[2, j]),
        )

    for j in range(heads):
        for copy in copies(j):
            copy.start()
    bias_out[...] = bias_final[0, :heads]
    for j in range(heads):
        for copy in copies(j):
            copy.wait()


def shards(queries, keys, values, out_grad, cross_bias, lengths):
    heads = cross_bias.shape[0]
    chips, convs = lax.axis_size("seq") // 2, lax.axis_size("dp")
    like = jax.ShapeDtypeStruct(queries.shape, BF)
    dma = pltpu.SemaphoreType.DMA
    anywhere = pl.BlockSpec(memory_space=pl.ANY)
    scalar = pl.BlockSpec(memory_space=pltpu.SMEM)
    tile = (BLOCK, BLOCK)
    wide = (BLOCK, 2 * BLOCK)
    vmem = pl.BlockSpec(memory_space=pltpu.VMEM)
    staged = pl.pallas_call(
        functools.partial(kernel, heads, chips, convs),
        out_shape=(
            pltpu.VMEM((heads, *tile), BF),
            pltpu.VMEM((heads, 2, *tile), BF),
            pltpu.VMEM((1, BLOCK), F32),
        ),
        in_specs=[scalar, scalar] + [anywhere] * 4,
        out_specs=(vmem, vmem, vmem),
        scratch_shapes=[
            pltpu.VMEM((WINDOW, heads, 2, *tile), BF),
            pltpu.VMEM((heads, 2, 2 * BLOCK, BLOCK), BF),
            pltpu.VMEM((2, *wide), F32),
            pltpu.VMEM((2, WINDOW, *wide), F32),
            pltpu.VMEM((2, WINDOW, *wide), F32),
            pltpu.VMEM((4, heads, 2, *tile), F32),
            pltpu.VMEM((3, heads, 2, *tile), BF),
            pltpu.VMEM((4, heads, 2, *tile), BF),
            pltpu.VMEM((3, heads, 2, *tile), BF),
            pltpu.VMEM((3, heads, 2, *tile), BF),
            pltpu.VMEM((heads, *tile), F32),
            pltpu.VMEM((heads, *tile), BF),
            pltpu.VMEM((heads, *tile), BF),
            pltpu.VMEM((heads, 8, 2 * BLOCK), F32),
            pltpu.VMEM((heads, 8, 2 * BLOCK), F32),
            pltpu.VMEM((heads, BLOCK), F32),
            pltpu.VMEM((heads, BLOCK), F32),
            pltpu.VMEM((chips, heads, BLOCK), F32),
            pltpu.VMEM((4, heads, BLOCK), F32),
            pltpu.VMEM((4, heads, BLOCK), F32),
            dma((4, heads)),
            dma((3, heads)),
            dma((3, heads)),
            dma((3, heads)),
            dma((3, heads)),
            dma((heads,)),
            dma((heads,)),
            dma((heads,)),
            dma((heads,)),
            dma((3, heads)),
            dma((4, heads)),
            dma((3, heads)),
            dma((3, heads)),
            dma((heads,)),
            dma((heads,)),
            dma((2,)),
            dma((chips,)),
            dma((chips,)),
            dma((4,)),
            dma((4,)),
            dma((4,)),
            dma((4,)),
        ],
        compiler_params=pltpu.CompilerParams(
            collective_id=0, has_side_effects=True, vmem_limit_bytes=56 * 1024 * 1024
        ),
    )(lengths, cross_bias, queries, keys, values, out_grad)
    return pl.pallas_call(
        functools.partial(publish, heads),
        out_shape=(like, like, like, jax.ShapeDtypeStruct((heads,), F32)),
        in_specs=[vmem, vmem, vmem],
        out_specs=(anywhere, anywhere, anywhere, vmem),
        scratch_shapes=[dma((3, heads))],
        compiler_params=pltpu.CompilerParams(vmem_limit_bytes=4 * 1024 * 1024),
    )(*staged)


def solution(mesh):
    split = P("dp", "chan", "seq", None)
    return jax.shard_map(
        shards,
        mesh=mesh,
        in_specs=(split, split, split, split, P(), P("dp")),
        out_specs=(split, split, split, P()),
        check_vma=False,
    )
```

```python
import functools
import math

import jax
import jax.numpy as jnp
from jax import lax
from jax.experimental import pallas as pl
from jax.experimental.pallas import tpu as pltpu
from jax.sharding import PartitionSpec as P

BLOCK = 128
WINDOW = 7
NEG_FILL = -1e30
MESH = pl.DeviceIdType.MESH
NT = (((1,), (1,)), ((), ()))
NN = (((1,), (0,)), ((), ()))
TN = (((0,), (0,)), ((), ()))
BF = jnp.bfloat16
F32 = jnp.float32


def dot(a, b, dims):
    return lax.dot_general(a, b, dims, preferred_element_type=F32)


def kernel(
    heads,
    chips,
    convs,
    lengths,
    bias,
    q_hbm,
    k_hbm,
    v_hbm,
    g_hbm,
    dq_stage,
    out_stage,
    bias_final,
    kv,
    qg,
    tri,
    prob,
    wgrad,
    terms,
    side_out,
    side_in,
    chain_out,
    chain_in,
    dq_own,
    dq_send,
    dq_recv,
    stat_out,
    stat_in,
    bias_out,
    bias_mate,
    bias_seq,
    bias_place,
    load_sem,
    hop_s,
    hop_r,
    side_s,
    side_r,
    swap_s,
    swap_r,
    stat_s,
    stat_r,
    term_s,
    term_r,
    chain_s,
    chain_r,
    dq_s,
    dq_r,
    mate_sem,
    seq_s,
    seq_r,
    place_s,
    place_r,
):
    root_scale = 1.0 / math.sqrt(BLOCK)
    chan = lax.axis_index("chan")
    seq = lax.axis_index("seq")
    chip = lax.div(seq, 2)
    core = lax.rem(seq, 2)
    mate = {"seq": seq + 1 - 2 * core}
    partner = {"chan": 1 - chan}
    above = {"seq": lax.rem(seq + 2, 2 * chips)}
    below = {"seq": lax.rem(seq + 2 * chips - 2, 2 * chips)}
    has_above = chip < chips - 1
    conv = lax.axis_index("dp")
    place = chan * convs + conv
    places = 2 * convs

    def chip_peer(k):
        there = lax.rem(chip + k, chips)
        return there, {"seq": 2 * there + core}

    def place_peer(k):
        there = lax.rem(place + k, places)
        return there, {"chan": lax.div(there, convs), "dp": lax.rem(there, convs)}

    groups = (
        (bias_seq, seq_s, seq_r, chip, chip_peer, chips),
        (bias_place, place_s, place_r, place, place_peer, places),
    )

    def remote(src, dst, send, recv, where):
        return pltpu.make_async_remote_copy(
            src_ref=src, dst_ref=dst, send_sem=send, recv_sem=recv, device_id=where, device_id_type=MESH
        )

    def loads(j):
        cols = pl.ds(pl.multiple_of(j * BLOCK, BLOCK), BLOCK)
        own = pl.ds(0, BLOCK)
        return (
            pltpu.make_async_copy(k_hbm.at[0, 0, :, cols], kv.at[0, j, 0], load_sem.at[0, j]),
            pltpu.make_async_copy(v_hbm.at[0, 0, :, cols], kv.at[0, j, 1], load_sem.at[1, j]),
            pltpu.make_async_copy(q_hbm.at[0, 0, :, cols], qg.at[j, 0, own], load_sem.at[2, j]),
            pltpu.make_async_copy(g_hbm.at[0, 0, :, cols], qg.at[j, 1, own], load_sem.at[3, j]),
        )

    def hop(n, j):
        return remote(kv.at[2 * n - 2, j], kv.at[2 * n, j], hop_s.at[n - 1, j], hop_r.at[n - 1, j], above)

    def side(n, j):
        i = n - core
        return remote(kv.at[2 * n, j], kv.at[2 * i + 1, j], side_s.at[i, j], side_r.at[i, j], mate)

    def side_arrival(i, j):
        return remote(kv.at[2 * i + 1, j], kv.at[2 * i + 1, j], side_s.at[i, j], side_r.at[i, j], mate)

    def swap(j):
        return remote(
            qg.at[j, :, pl.ds(0, BLOCK)], qg.at[j, :, pl.ds(BLOCK, BLOCK)], swap_s.at[j], swap_r.at[j], partner
        )

    def stat(j):
        return remote(stat_out.at[j], stat_in.at[j], stat_s.at[j], stat_r.at[j], partner)

    def term(i, j):
        h = i + 1 - core
        return remote(side_out.at[i, j], side_in.at[h, j], term_s.at[i, j], term_r.at[h, j], mate)

    def term_arrival(h, j):
        return remote(side_in.at[h, j], side_in.at[h, j], term_s.at[0, j], term_r.at[h, j], mate)

    def chain(h, j):
        return remote(
            chain_out.at[h - 1, j], chain_in.at[h - 1, j], chain_s.at[h - 1, j], chain_r.at[h - 1, j], below
        )

    def query(j):
        return remote(dq_send.at[j], dq_recv.at[j], dq_s.at[j], dq_r.at[j], partner)

    def fetch(j, _):
        for copy in loads(j):
            copy.start()
        return 0

    lax.fori_loop(0, heads, fetch, 0)

    barrier = pltpu.get_barrier_semaphore()
    pl.semaphore_signal(barrier, inc=1, device_id=mate, device_id_type=MESH)
    for *_, peer, size in groups:
        for k in range(1, size):
            pl.semaphore_signal(barrier, inc=1, device_id=peer(k)[1], device_id_type=MESH)

    key_row = lax.broadcasted_iota(jnp.int32, (BLOCK, 2 * BLOCK), 0)
    query_col = lax.rem(lax.broadcasted_iota(jnp.int32, (BLOCK, 2 * BLOCK), 1), BLOCK)
    absent = [jnp.where(seq >= d, 0.0, NEG_FILL).astype(F32) for d in range(WINDOW)]
    tri[0] = jnp.where(key_row <= query_col, 0.0, NEG_FILL)
    tri[1] = jnp.where(key_row > query_col, 0.0, NEG_FILL) + absent[WINDOW - 1]
    lane = lax.rem(lax.broadcasted_iota(jnp.int32, (1, 2 * BLOCK), 1), BLOCK)
    valid = jnp.where(seq * BLOCK + lane < lengths[0], 1.0, 0.0).astype(F32)
    crossed = lax.broadcasted_iota(jnp.int32, (1, 2 * BLOCK), 1) >= BLOCK

    def clear(j, _):
        nothing = jnp.zeros((2, BLOCK, BLOCK), BF)
        for d in range(1, WINDOW):

            @pl.when(seq < d)
            def _():
                kv[d, j] = nothing

        @pl.when(core == 0)
        def _():
            side_in[3, j] = nothing

        @pl.when(core == 1)
        def _():
            side_in[0, j] = nothing

        @pl.when(jnp.logical_not(has_above))
        def _():
            for h in range(3):
                chain_in[h, j] = nothing

        return 0

    lax.fori_loop(0, heads, clear, 0)

    pl.semaphore_wait(barrier, chips + places - 1)

    def forward(j):
        swap(j).wait_recv()
        for i in range(3):

            @pl.when(seq >= 2 * i + 1)
            def _():
                side_arrival(i, j).wait_recv()

        queries, grads = qg[j, 0], qg[j, 1]
        slot = lax.rem(j, 2)
        peak = None
        for d in range(WINDOW):
            score = dot(kv[d, j, 0], queries, NT) * root_scale
            if d == 0:
                score = score + tri[0]
            elif d == WINDOW - 1:
                score = score + tri[1]
            else:
                score = score + absent[d]
            prob[slot, d] = score
            top = jnp.max(score, axis=0, keepdims=True)
            peak = top if peak is None else jnp.maximum(peak, top)
        total = moment = None
        for d in range(WINDOW):
            weight_grad = dot(kv[d, j, 1], grads, NT)
            weight = jnp.exp(prob[slot, d] - peak)
            prob[slot, d] = weight
            wgrad[slot, d] = weight_grad
            a = jnp.sum(weight, axis=0, keepdims=True)
            b = jnp.sum(weight * weight_grad, axis=0, keepdims=True)
            total = a if total is None else total + a
            moment = b if moment is None else moment + b
        offset = jnp.where(crossed, bias[j], 0.0)
        stat_out[j, 0:1] = peak + offset
        stat_out[j, 1:2] = total
        stat_out[j, 2:3] = moment
        stat_out[j, 3:8] = jnp.zeros((5, 2 * BLOCK), F32)
        stat(j).start()

    def backward(j):
        stat(j).wait_recv()

        def turned(row):
            theirs = stat_in[j, row : row + 1]
            return jnp.concatenate([theirs[:, BLOCK:], theirs[:, :BLOCK]], axis=1)

        peak = stat_out[j, 0:1]
        their_peak = turned(0)
        merged = jnp.maximum(peak, their_peak)
        mine, theirs = jnp.exp(peak - merged), jnp.exp(their_peak - merged)
        own_total = stat_out[j, 1:2] * mine
        own_moment = stat_out[j, 2:3] * mine
        inverse = valid / (own_total + turned(1) * theirs)
        delta = (own_moment + turned(2) * theirs) * inverse
        rescale = mine * inverse
        offset_term = (own_moment - delta * own_total) * inverse
        bias_out[pl.ds(j, 1), :] = offset_term[:, BLOCK:]

        @pl.when(j == heads - 1)
        def _():
            bias_out[...] = jnp.broadcast_to(jnp.sum(bias_out[...], axis=1, keepdims=True), bias_out.shape)
            mate_total().start()

        queries, grads = qg[j, 0], qg[j, 1]
        slot = lax.rem(j, 2)
        query_term = None
        for d in range(WINDOW):
            weight = prob[slot, d] * rescale
            score_grad = (weight * (wgrad[slot, d] - delta)).astype(BF)
            weight = weight.astype(BF)
            value_term = dot(weight, grads, NN)
            key_term = dot(score_grad, queries, NN) * root_scale
            part = dot(score_grad, kv[d, j, 0], TN)
            query_term = part if query_term is None else query_term + part
            if d % 2 == 0:
                terms[d // 2, j, 0] = key_term
                terms[d // 2, j, 1] = value_term
            else:
                side_out[d // 2, j, 0] = key_term.astype(BF)
                side_out[d // 2, j, 1] = value_term.astype(BF)
        query_term = query_term * root_scale
        dq_own[j] = query_term[:BLOCK]
        dq_send[j] = query_term[BLOCK:].astype(BF)
        for i in range(3):

            @pl.when(seq >= 2 * i + 1)
            def _():
                term(i, j).start()

        query(j).start()

    def mate_total():
        return remote(bias_out, bias_mate, mate_sem.at[0], mate_sem.at[1], mate)

    def spread(group):
        ref, send, recv, mine, peer, size = groups[group]
        for k in range(1, size):
            remote(ref.at[mine], ref.at[mine], send.at[k], recv.at[mine], peer(k)[1]).start()

    def gather(group):
        ref, send, recv, mine, peer, size = groups[group]
        for k in range(1, size):
            there, where = peer(k)
            remote(ref.at[there], ref.at[there], send.at[k], recv.at[there], where).wait_recv()
        return functools.reduce(jnp.add, [ref[n] for n in range(size)])

    def bias_stage(n):
        if n == 0:
            mate_total().wait_recv()
            bias_seq[chip] = bias_out[...] + bias_mate[...]
            spread(0)
        elif n == 1:
            bias_place[place] = gather(0)
            spread(1)
        else:
            bias_mate[...] = gather(1)

    def within(j, action):
        @pl.when(jnp.logical_and(j >= 0, j < heads))
        def _():
            action(j)

    def send_own(j):
        for copy in loads(j):
            copy.wait()

        @pl.when(has_above)
        def _():
            hop(1, j).start()

        @pl.when(core == 0)
        def _():
            side(0, j).start()

        swap(j).start()

    def relay(n, j):
        @pl.when(chip >= n)
        def _():
            hop(n, j).wait_recv()
            if n < 3:

                @pl.when(has_above)
                def _():
                    hop(n + 1, j).start()

                side(n, j).start()
            else:

                @pl.when(core == 1)
                def _():
                    side(n, j).start()

    def finish_query(j):
        query(j).wait_recv()
        dq_stage[j] = (dq_own[j] + dq_recv[j].astype(F32)).astype(BF)

    def reduce(h, j):
        @pl.when(chip >= h)
        def _():
            if h == 3:
                pl.when(core == 1)(lambda: term_arrival(h, j).wait_recv())
            elif h == 0:
                pl.when(core == 0)(lambda: term_arrival(h, j).wait_recv())
            else:
                term_arrival(h, j).wait_recv()
            total = terms[h, j] + side_in[h, j].astype(F32)
            if h < 3:
                pl.when(has_above)(lambda: chain(h + 1, j).wait_recv())
                total = total + chain_in[h, j].astype(F32)
            if h > 0:
                chain_out[h - 1, j] = total.astype(BF)
                chain(h, j).start()
            else:
                out_stage[j] = total.astype(BF)

    def step(i, _):
        within(i + 2, functools.partial(relay, 1))
        within(i + 1, functools.partial(relay, 2))
        within(i + 4, send_own)
        within(i, functools.partial(relay, 3))
        within(i - 4, functools.partial(reduce, 2))
        within(i - 5, functools.partial(reduce, 1))
        within(i - 2, functools.partial(reduce, 3))
        within(i - 6, functools.partial(reduce, 0))
        within(i, forward)
        within(i - 1, backward)
        within(i - 3, finish_query)
        for n in range(3):
            pl.when(i == heads + 1 + n)(functools.partial(bias_stage, n))
        return 0

    lax.fori_loop(-4, heads + 6, step, 0)

    def drain(j, _):
        swap(j).wait_send()
        stat(j).wait_send()
        query(j).wait_send()
        for n in range(1, 4):
            pl.when(jnp.logical_and(has_above, chip >= n - 1))(lambda: hop(n, j).wait_send())
        pl.when(core == 0)(lambda: side(0, j).wait_send())
        for n in (1, 2):
            pl.when(chip >= n)(lambda: side(n, j).wait_send())
        pl.when(jnp.logical_and(chip >= 3, core == 1))(lambda: side(3, j).wait_send())
        for i in range(3):
            pl.when(seq >= 2 * i + 1)(lambda: term(i, j).wait_send())
        for h in range(1, 4):
            pl.when(chip >= h)(lambda: chain(h, j).wait_send())
        return 0

    lax.fori_loop(0, heads, drain, 0)
    mate_total().wait_send()
    for ref, send, recv, mine, peer, size in groups:
        for k in range(1, size):
            remote(ref.at[mine], ref.at[mine], send.at[k], recv.at[mine], peer(k)[1]).wait_send()
    head_row = lax.broadcasted_iota(jnp.int32, (heads, BLOCK), 0)
    head_lane = lax.broadcasted_iota(jnp.int32, (heads, BLOCK), 1)
    picked = jnp.where(head_row == head_lane, bias_mate[...], 0.0)
    bias_final[...] = jnp.sum(picked, axis=0, keepdims=True)


def publish(heads, dq_stage, out_stage, bias_final, dq_hbm, dk_hbm, dv_hbm, bias_out, sem):
    def copies(j):
        cols = pl.ds(pl.multiple_of(j * BLOCK, BLOCK), BLOCK)
        return (
            pltpu.make_async_copy(dq_stage.at[j], dq_hbm.at[0, 0, :, cols], sem.at[0, j]),
            pltpu.make_async_copy(out_stage.at[j, 0], dk_hbm.at[0, 0, :, cols], sem.at[1, j]),
            pltpu.make_async_copy(out_stage.at[j, 1], dv_hbm.at[0, 0, :, cols], sem.at[2, j]),
        )

    for j in range(heads):
        for copy in copies(j):
            copy.start()
    bias_out[...] = bias_final[0, :heads]
    for j in range(heads):
        for copy in copies(j):
            copy.wait()


def shards(queries, keys, values, out_grad, cross_bias, lengths):
    heads = cross_bias.shape[0]
    chips, convs = lax.axis_size("seq") // 2, lax.axis_size("dp")
    like = jax.ShapeDtypeStruct(queries.shape, BF)
    dma = pltpu.SemaphoreType.DMA
    anywhere = pl.BlockSpec(memory_space=pl.ANY)
    scalar = pl.BlockSpec(memory_space=pltpu.SMEM)
    tile = (BLOCK, BLOCK)
    wide = (BLOCK, 2 * BLOCK)
    vmem = pl.BlockSpec(memory_space=pltpu.VMEM)
    staged = pl.pallas_call(
        functools.partial(kernel, heads, chips, convs),
        out_shape=(
            pltpu.VMEM((heads, *tile), BF),
            pltpu.VMEM((heads, 2, *tile), BF),
            pltpu.VMEM((1, BLOCK), F32),
        ),
        in_specs=[scalar, scalar] + [anywhere] * 4,
        out_specs=(vmem, vmem, vmem),
        scratch_shapes=[
            pltpu.VMEM((WINDOW, heads, 2, *tile), BF),
            pltpu.VMEM((heads, 2, 2 * BLOCK, BLOCK), BF),
            pltpu.VMEM((2, *wide), F32),
            pltpu.VMEM((2, WINDOW, *wide), F32),
            pltpu.VMEM((2, WINDOW, *wide), F32),
            pltpu.VMEM((4, heads, 2, *tile), F32),
            pltpu.VMEM((3, heads, 2, *tile), BF),
            pltpu.VMEM((4, heads, 2, *tile), BF),
            pltpu.VMEM((3, heads, 2, *tile), BF),
            pltpu.VMEM((3, heads, 2, *tile), BF),
            pltpu.VMEM((heads, *tile), F32),
            pltpu.VMEM((heads, *tile), BF),
            pltpu.VMEM((heads, *tile), BF),
            pltpu.VMEM((heads, 8, 2 * BLOCK), F32),
            pltpu.VMEM((heads, 8, 2 * BLOCK), F32),
            pltpu.VMEM((heads, BLOCK), F32),
            pltpu.VMEM((heads, BLOCK), F32),
            pltpu.VMEM((chips, heads, BLOCK), F32),
            pltpu.VMEM((2 * convs, heads, BLOCK), F32),
            dma((4, heads)),
            dma((3, heads)),
            dma((3, heads)),
            dma((3, heads)),
            dma((3, heads)),
            dma((heads,)),
            dma((heads,)),
            dma((heads,)),
            dma((heads,)),
            dma((3, heads)),
            dma((4, heads)),
            dma((3, heads)),
            dma((3, heads)),
            dma((heads,)),
            dma((heads,)),
            dma((2,)),
            dma((chips,)),
            dma((chips,)),
            dma((2 * convs,)),
            dma((2 * convs,)),
        ],
        compiler_params=pltpu.CompilerParams(
            collective_id=0, has_side_effects=True, vmem_limit_bytes=56 * 1024 * 1024
        ),
    )(lengths, cross_bias, queries, keys, values, out_grad)
    return pl.pallas_call(
        functools.partial(publish, heads),
        out_shape=(like, like, like, jax.ShapeDtypeStruct((heads,), F32)),
        in_specs=[vmem, vmem, vmem],
        out_specs=(anywhere, anywhere, anywhere, vmem),
        scratch_shapes=[dma((3, heads))],
        compiler_params=pltpu.CompilerParams(vmem_limit_bytes=4 * 1024 * 1024),
    )(*staged)


def solution(mesh):
    split = P("dp", "chan", "seq", None)
    return jax.shard_map(
        shards,
        mesh=mesh,
        in_specs=(split, split, split, split, P(), P("dp")),
        out_specs=(split, split, split, P()),
        check_vma=False,
    )
```
